256 devices in a mesh: seq: 16 (over y, x_lo, core), exp: 16 (over z, x_hi).
Axes of the slice: x: 4 (x_hi: 2, x_lo: 2; x = x_hi * 2 + x_lo), y: 4, z: 8, core: 2. Of those that a mesh axis runs over, the one named last changes fastest.
Arguments:
- queries: bfloat16 [4096, 4096], P('seq', 'exp'), may hold values from -6 to 6
- key_rows: bfloat16 [4096, 512], P('seq'), may hold values from -6 to 6
- value_rows: bfloat16 [4096, 512], P('seq'), may hold values from -6 to 6
- sink_logits: float32 [64], P('exp'), may hold values from -2 to 2
- residual: bfloat16 [4096, 2880], P('seq'), may hold values from -6 to 6
- out_weight: bfloat16 [4096, 2880], P('exp'), may hold values from -0.375 to 0.375
- norm_gain: float32 [2880], replicated, may hold values from 0.25 to 1.75
- expert_ids: int32 [4096, 4], P('seq'), may hold values from 0 to 63, all different within a row; in each aligned block of 256 rows (0 to 255, 256 to 511, ...) at most 24 rows name the same one
- route_gates: float32 [4096, 4], P('seq'), may hold values from 0.1 to 0.6
- gate_proj: bfloat16 [64, 2880, 2048], P('seq', None, 'exp'), may hold values from -0.109375 to 0.109375
- up_proj: bfloat16 [64, 2880, 2048], P('seq', None, 'exp'), may hold values from -0.109375 to 0.109375
- down_proj: bfloat16 [64, 2048, 2880], P('seq', 'exp'), may hold values from -0.125 to 0.125
Outputs:
- layer_out: bfloat16 [4096, 2880], P('seq')
The draws below stay inside these ranges and needn't reach their ends.
Inputs may be any that keep to these rules, and one draw needn't show every extreme that they name: `expert_ids`: each token names 4 different experts. In each slab of 256 tokens no expert is named by more than 24 entries, and that bound is reached.
All inputs are finite; a program needn't handle non-finite values.
Results may differ from the reference program's by a relative error of at most 0.018.
Values may be sent and summed in bfloat16 or wider, within the bound.
A program may use at most 128 MiB of HBM per device.

```python
import math
import jax
import jax.numpy as jnp
import numpy as np
from jax import lax

D = 2880
HQ = 64
HK = 8
HEAD = 64
TOP = 4
WIN = 128
FF = 2048
SLAB = 256
SEQ_LEN = 4096
EXPERTS = 64
CAP = 24
N_EXP = 16


def draw_queries(key, part):
    base_key = jax.random.fold_in(key, 1)
    fresh = jnp.clip(jax.random.normal(base_key, (SEQ_LEN, HQ * HEAD), jnp.float32), -4.0, 4.0)
    return fresh.astype(jnp.bfloat16)


def draw_key_rows(key, part):
    base_key = jax.random.fold_in(key, 2)
    fresh = jnp.clip(jax.random.normal(base_key, (SEQ_LEN, HK * HEAD), jnp.float32), -4.0, 4.0)
    return fresh.astype(jnp.bfloat16)


def steps_of(key, dims, shards, low, top_value):
    loudness, own = 1.0, jax.random.fold_in(key, 6)
    for axis_at, shards_of in shards:
        draws = jnp.exp(jax.random.uniform(jax.random.fold_in(own, axis_at), (shards_of,), jnp.float32, low / len(shards), top_value / len(shards)))
        loudness = loudness * jnp.repeat(draws, dims[axis_at] // shards_of).reshape([-1 if axis == axis_at else 1 for axis in range(len(dims))])
    return loudness


def shared_out(own_key, own, number, rows, amount, top, bound, lean):
    sequence = jax.random.permutation(own_key, amount)
    packed, usual = shares(amount, rows * top, bound, lean, True), shares(amount, rows * top, bound, lean, False)
    places = jnp.arange(amount)

    def named(lengths, rotation):
        used = int((lengths > 0).sum())
        fixed = max(1, used // 4)
        passed = fixed + (places - fixed + rotation * (used - fixed)) % max(1, amount - fixed)
        return jnp.zeros((amount,), jnp.int32).at[sequence[jnp.where(places < fixed, places, passed)]].set(jnp.asarray(lengths, jnp.int32))

    lengths = jnp.where(number % 4 == 0, named(packed, number // 4), named(usual, number - number // 4 - 1))
    mixed = jax.random.permutation(jax.random.fold_in(own, 3), amount)
    source_of, sink = mixed[0:amount // 2 * 2:2], mixed[1:amount // 2 * 2:2]
    margin = jnp.minimum(lengths[source_of] - 1, bound - lengths[sink]) // 2
    margin = jnp.where((source_of == sequence[0]) | (sink == sequence[0]) | (lengths[sink] == 0), 0, jnp.maximum(margin, 0))
    passed = jax.random.randint(jax.random.fold_in(own, 4), (amount // 2,), 0, 1 << 20) % (margin + 1)
    lengths = lengths.at[source_of].add(-passed).at[sink].add(passed)
    members = jnp.searchsorted(jnp.cumsum(lengths), jnp.arange(rows * top), side="right").astype(jnp.int32)
    table = members.reshape(top, rows).T
    table = table[jax.random.permutation(jax.random.fold_in(own, 1), rows)]
    rotation = jax.random.randint(jax.random.fold_in(own, 2), (rows, 1), 0, top)
    return jnp.take_along_axis(table, (jnp.arange(top)[None, :] + rotation) % top, axis=1)


def shares(number_of, total, bound, lean, full):
    portions = [(1 << 20) // math.isqrt(grade ** lean) + 1 for grade in range(1, number_of + 1)]
    largest = bound if full else min(bound, max(-(-total // number_of), total * portions[0] // sum(portions)))
    least = 1 if total - largest >= number_of - 1 else 0
    holding, surplus = [largest] + [least] * (number_of - 1), total - largest - least * (number_of - 1)
    while surplus > 0:
        candidates = [i for i in range(1, number_of) if holding[i] < largest] or [i for i in range(1, number_of) if holding[i] < bound]
        whole, left = sum([portions[i] for i in candidates]), surplus
        for i in candidates:
            more = min(bound - holding[i], max(1, left * portions[i] // whole), surplus)
            holding[i] = holding[i] + more
            surplus = surplus - more
    return np.array(holding)


def normal_values(rng, shape, width, reach, cuts=(), kind=jnp.bfloat16):
    entries = width * jax.random.normal(rng, shape, jnp.float32)
    if cuts:
        entries = entries * steps_of(rng, shape, cuts, -0.22, 0.18)
    return jnp.clip(entries, -reach, reach).astype(kind)


def setup_inputs(seed: int = 0) -> dict:
    splits = jax.random.split(jax.random.key(seed), 13)
    queries = draw_queries(jax.random.fold_in(splits[12], 71), 0)
    key_rows = draw_key_rows(jax.random.fold_in(splits[12], 71), 0)
    value_rows = normal_values(splits[2], (SEQ_LEN, HK * HEAD), 1.0, 6.0, ((0, 16),))
    sink_logits = jnp.clip(jax.random.uniform(splits[3], (HQ,), jnp.float32, -2.0, 2.0) * steps_of(splits[3], (HQ,), ((0, 16),), -0.4, 0.0), -2.0, 2.0)
    residual = normal_values(splits[4], (SEQ_LEN, D), 1.0, 6.0, ((0, 16),))
    out_weight = normal_values(splits[5], (HQ * HEAD, D), (HQ * HEAD // 16) ** -0.5, 0.375, ((0, 16),))
    norm_gain = jnp.clip(1.0 + 0.15 * jax.random.normal(splits[6], (D,), jnp.float32), 0.25, 1.75)
    expert_ids_keys = jax.random.split(jax.random.fold_in(splits[7], 1), SEQ_LEN // SLAB)
    expert_ids_turns = jax.random.permutation(jax.random.fold_in(splits[7], 3), SEQ_LEN // SLAB)
    expert_ids = jax.vmap(lambda own, number: shared_out(jax.random.fold_in(splits[7], 2), own, number, SLAB, EXPERTS, TOP, CAP, 2))(expert_ids_keys, expert_ids_turns).reshape((SEQ_LEN, TOP))
    route_gates = jnp.clip(0.1 + 0.5 * jax.random.uniform(splits[8], (SEQ_LEN, TOP), jnp.float32) ** steps_of(splits[8], (SEQ_LEN, TOP), ((0, 16),), -0.2, 0.2), 0.1, 0.6)
    gate_proj = normal_values(splits[9], (EXPERTS, D, FF), D ** -0.5, 0.109375, ((0, 16), (2, 16)))
    up_proj = normal_values(splits[10], (EXPERTS, D, FF), D ** -0.5, 0.109375, ((0, 16), (2, 16)))
    down_proj = normal_values(splits[11], (EXPERTS, FF, D), FF ** -0.5, 0.125, ((0, 16), (1, 16)))
    return dict(queries=queries, key_rows=key_rows, value_rows=value_rows, sink_logits=sink_logits, residual=residual, out_weight=out_weight, norm_gain=norm_gain, expert_ids=expert_ids, route_gates=route_gates, gate_proj=gate_proj, up_proj=up_proj, down_proj=down_proj)


def normalize(mixed, gain):
    wide_vals = mixed.astype(jnp.float32)
    inv_scale = lax.rsqrt(lax.optimization_barrier(jnp.mean(wide_vals * wide_vals, axis=-1, keepdims=True)) + 1e-05)
    return (wide_vals * inv_scale * gain).astype(jnp.bfloat16)

def activate(gate_acc, up_acc):
    gate_acc = jnp.minimum(gate_acc, 7.0)
    up_acc = jnp.clip(up_acc, -7.0, 7.0)
    return ((up_acc + 1.0) * gate_acc * jax.nn.sigmoid(1.702 * gate_acc)).astype(jnp.bfloat16)

def slot_numbers(flat_ids, experts):
    onehot = (flat_ids[:, None] == jnp.arange(experts, dtype=jnp.int32)[None, :]).astype(jnp.int32)
    rank_ids = jnp.cumsum(onehot, axis=0) - 1
    return lax.optimization_barrier(jnp.sum(rank_ids * onehot, axis=1)).astype(jnp.int32)

def reference(queries, key_rows, value_rows, sink_logits, residual, out_weight, norm_gain, expert_ids, route_gates, gate_proj, up_proj, down_proj):
    per_group = HQ // HK
    slab_count = SEQ_LEN // SLAB
    q_slabs = queries.reshape(slab_count, SLAB, HQ, HEAD)
    k_slabs = key_rows.reshape(slab_count, SLAB, HK, HEAD)
    v_slabs = value_rows.reshape(slab_count, SLAB, HK, HEAD)
    zero_tail = jnp.zeros((1, WIN, HK, HEAD), jnp.bfloat16)
    k_full = jnp.concatenate([jnp.concatenate([zero_tail, k_slabs[:-1, SLAB - WIN:]], 0), k_slabs], 1)
    v_full = jnp.concatenate([jnp.concatenate([zero_tail, v_slabs[:-1, SLAB - WIN:]], 0), v_slabs], 1)
    factor = 1.0 / math.sqrt(HEAD)

    def one_slab(inputs):
        q_block, k_block, v_block, first_pos = inputs
        k_heads = jnp.repeat(k_block, per_group, axis=1).astype(jnp.float32)
        v_heads = jnp.repeat(v_block, per_group, axis=1).astype(jnp.float32)
        scores = jnp.einsum('qhd,khd->hqk', q_block.astype(jnp.float32), k_heads) * factor
        q_pos = first_pos + jnp.arange(SLAB, dtype=jnp.int32)
        k_pos = first_pos - WIN + jnp.arange(WIN + SLAB, dtype=jnp.int32)
        allowed = (k_pos[None, :] <= q_pos[:, None]) & (k_pos[None, :] > q_pos[:, None] - WIN) & (k_pos[None, :] >= 0)
        scores = jnp.where(allowed[None], scores, -1e+30)
        row_top = jnp.maximum(lax.optimization_barrier(jnp.max(scores, axis=-1)), sink_logits[:, None])
        expo = jnp.exp(scores - row_top[..., None])
        denominator = lax.optimization_barrier(jnp.sum(expo, axis=-1)) + jnp.exp(sink_logits[:, None] - row_top)
        weights = (expo / denominator[..., None]).astype(jnp.bfloat16)
        context = jnp.einsum('hqk,khd->qhd', weights.astype(jnp.float32), v_heads)
        return context.astype(jnp.bfloat16).reshape(SLAB, HQ * HEAD)
    starts = jnp.arange(slab_count, dtype=jnp.int32) * SLAB
    context = lax.map(one_slab, (q_slabs, k_full, v_full, starts)).reshape(SEQ_LEN, HQ * HEAD)
    attn_out = jnp.dot(context, out_weight, preferred_element_type=jnp.float32)
    mixed = (residual.astype(jnp.float32) + attn_out).astype(jnp.bfloat16)
    normed = normalize(mixed, norm_gain)
    flat_ids = expert_ids.reshape(slab_count, SLAB * TOP).astype(jnp.int32)
    slot_ids = jax.vmap(lambda row_ids: slot_numbers(row_ids, EXPERTS))(flat_ids)
    token_of = jnp.arange(SLAB * TOP, dtype=jnp.int32) // TOP
    source_ids = jnp.arange(slab_count, dtype=jnp.int32)[:, None]
    target_rows = ((flat_ids * slab_count + source_ids) * CAP + slot_ids).reshape(-1)
    normed_slabs = normed.reshape(slab_count, SLAB, D)
    entry_rows = normed_slabs[:, token_of].reshape(-1, D)
    buffer = jnp.zeros((EXPERTS * slab_count * CAP, D), jnp.bfloat16).at[target_rows].set(entry_rows)
    buffer = buffer.reshape(EXPERTS, slab_count * CAP, D)
    blocks = FF // N_EXP

    def one_expert(inputs):
        slot_rows, w_gate, w_up, w_down = inputs
        gate_acc = jnp.dot(slot_rows, w_gate, preferred_element_type=jnp.float32)
        up_acc = jnp.dot(slot_rows, w_up, preferred_element_type=jnp.float32)
        hidden = activate(gate_acc, up_acc)
        hidden_blocks = hidden.reshape(-1, N_EXP, blocks).astype(jnp.float32)
        down_blocks = w_down.reshape(N_EXP, blocks, D).astype(jnp.float32)
        parts = jnp.einsum('rbf,bfd->brd', hidden_blocks, down_blocks).astype(jnp.bfloat16)
        parts = lax.optimization_barrier(parts)
        return lax.optimization_barrier(jnp.sum(parts.astype(jnp.float32), axis=0))
    expert_out = lax.map(one_expert, (buffer, gate_proj, up_proj, down_proj)).reshape(-1, D)
    picked = expert_out[target_rows].reshape(SEQ_LEN, TOP, D)
    moe = lax.optimization_barrier(jnp.sum(picked * route_gates[:, :, None], axis=1))
    return (mixed.astype(jnp.float32) + moe).astype(jnp.bfloat16)
```

```python
import functools
import math

import jax
import jax.numpy as jnp
from jax import lax
from jax.experimental import pallas as pl
from jax.experimental.pallas import tpu as pltpu
from jax.sharding import PartitionSpec as P

HQ = 64
HK = 8
HEAD = 64
TOP = 4
WIN = 128
NS = 16
NE = 16
EXPERTS = 64
CAP = 24
SLOTS = 2 * CAP
QUAD = 4
MESH = pl.DeviceIdType.MESH
BF = jnp.bfloat16
F32 = jnp.float32


def passed_along(x, axis, by):
    count = lax.axis_size(axis)
    pairs = [(i, i + by) for i in range(count) if 0 <= i + by < count]
    return lax.ppermute(x, axis, pairs)


def attention(queries, key_rows, value_rows, sink_logits, out_weight):
    tok_rows = queries.shape[0]
    local_heads = queries.shape[1] // HEAD
    per_group = HQ // HK
    column = lax.axis_index("exp")
    slab_index = lax.axis_index("seq")
    kv_start = column * local_heads // per_group
    key_own = lax.dynamic_slice_in_dim(key_rows, kv_start * HEAD, HEAD, 1)
    value_own = lax.dynamic_slice_in_dim(value_rows, kv_start * HEAD, HEAD, 1)
    both = jnp.concatenate([key_own, value_own], 1)
    tail = passed_along(both[tok_rows - WIN :], "seq", 1)
    full = jnp.concatenate([tail, both], 0)
    key_full, value_full = full[:, :HEAD], full[:, HEAD:]
    query_heads = queries.reshape(tok_rows, local_heads, HEAD)
    scores = jnp.einsum("qhd,kd->hqk", query_heads, key_full, preferred_element_type=F32) * (
        1.0 / math.sqrt(HEAD)
    )
    first_pos = slab_index * tok_rows
    q_pos = first_pos + jnp.arange(tok_rows, dtype=jnp.int32)
    k_pos = first_pos - WIN + jnp.arange(WIN + tok_rows, dtype=jnp.int32)
    allowed = (
        (k_pos[None, :] <= q_pos[:, None])
        & (k_pos[None, :] > q_pos[:, None] - WIN)
        & (k_pos[None, :] >= 0)
    )
    scores = jnp.where(allowed[None], scores, -1e30)
    row_top = jnp.maximum(jnp.max(scores, axis=-1), sink_logits[:, None])
    expo = jnp.exp(scores - row_top[..., None])
    denominator = jnp.sum(expo, axis=-1) + jnp.exp(sink_logits[:, None] - row_top)
    weights = (expo / denominator[..., None]).astype(BF)
    context = jnp.einsum("hqk,kd->qhd", weights, value_full, preferred_element_type=F32)
    context = context.astype(BF).reshape(tok_rows, local_heads * HEAD)
    return jnp.dot(context, out_weight, preferred_element_type=F32).astype(BF)


def routing(expert_ids, route_gates, parity):
    rows = expert_ids.shape[0]
    half = EXPERTS // 2
    ids = jnp.arange(half, dtype=jnp.int32)
    mine = (ids // 2) * 4 + 2 * parity + ids % 2
    hits = expert_ids[:, :, None] == mine[None, None, :]
    named = jnp.sum(hits.astype(F32), axis=1)
    gate_of = jnp.sum(jnp.where(hits, route_gates[:, :, None], 0.0), axis=1)
    earlier = (jnp.arange(rows)[:, None] > jnp.arange(rows)[None, :]).astype(BF)
    count = jnp.dot(earlier, named.astype(BF), preferred_element_type=F32)
    slot_of = jnp.where(named > 0, count, -1.0).astype(BF)
    columns = jnp.arange(half * CAP, dtype=jnp.int32)
    spread = (columns[None, :] // CAP == ids[:, None]).astype(BF)
    slot_wide = jnp.dot(slot_of, spread, preferred_element_type=F32)
    taken = slot_wide == (columns % CAP).astype(F32)[None, :]
    gate_wide = jnp.dot(gate_of.astype(BF), spread, preferred_element_type=F32)
    combine = jnp.where(taken, gate_wide, 0.0).astype(BF)
    pick = taken.astype(BF).T
    quad_cols = QUAD * SLOTS
    combine = combine.reshape(rows, -1, quad_cols).transpose(1, 0, 2)
    return pick.reshape(-1, quad_cols, rows), combine


def layer_kernel(
    attn_ref,
    resid_ref,
    gain_ref,
    pick_ref,
    comb_ref,
    gate_ref,
    up_ref,
    down_ref,
    out_ref,
    parts,
    parts2,
    normed,
    mixed,
    packed,
    arrived,
    outgoing,
    returned,
    w_in,
    w_down,
    total,
    moe_part,
    w_local,
    w_send,
    w_recv,
    rs_send,
    rs_recv,
    ag_send,
    ag_recv,
    di_send,
    di_recv,
    re_send,
    re_recv,
    rs2_send,
    rs2_recv,
    ag2_send,
    ag2_recv,
    own_sem,
):
    s = lax.axis_index("seq")
    e = lax.axis_index("exp")
    parity = lax.rem(lax.div(e, 2), 2)
    partner = e + 2 - 4 * parity
    rows = normed.shape[0] // NE
    quad = lax.div(s, QUAD)
    hid = down_ref.shape[1]

    barrier = pltpu.get_barrier_semaphore()

    @pl.loop(1, NE)
    def _(d):
        pl.semaphore_signal(
            barrier, inc=1, device_id={"exp": lax.rem(e + d, NE)}, device_id_type=MESH
        )

    @pl.loop(1, NS)
    def _(d):
        pl.semaphore_signal(
            barrier, inc=1, device_id={"seq": lax.rem(s + d, NS)}, device_id_type=MESH
        )

    pl.semaphore_wait(barrier, NE + NS - 2)

    def rdma(src, dst, send, recv, **where):
        return pltpu.make_async_remote_copy(
            src_ref=src,
            dst_ref=dst,
            send_sem=send,
            recv_sem=recv,
            device_id=where,
            device_id_type=MESH,
        )

    def exp_block(i):
        return pl.ds(pl.multiple_of(i * rows, rows), rows)

    def rs_copy(src, dst, send, recv, to, frm):
        return rdma(src.at[exp_block(to)], dst.at[frm], send.at[to], recv.at[frm], exp=to)

    @pl.loop(1, NE)
    def _(d):
        to = lax.rem(e + d, NE)
        rs_copy(attn_ref, parts, rs_send, rs_recv, to, e).start()

    own = pltpu.make_async_copy(attn_ref.at[exp_block(e)], parts.at[e], own_sem.at[0])
    own.start()

    w_own, w_out = [], []
    for k in range(2):
        for j, ref in enumerate((gate_ref, up_ref)):
            col = k * 4 * hid + j * 2 * hid
            w_own.append((ref.at[2 * parity + k], w_in.at[:, pl.ds(col, hid)]))
            w_out.append((ref.at[2 - 2 * parity + k], w_in.at[:, pl.ds(col + hid, hid)]))
        row = k * 2 * hid
        w_own.append((down_ref.at[2 * parity + k], w_down.at[pl.ds(row, hid)]))
        w_out.append((down_ref.at[2 - 2 * parity + k], w_down.at[pl.ds(row + hid, hid)]))
    w_own = [pltpu.make_async_copy(a, b, w_local.at[i]) for i, (a, b) in enumerate(w_own)]
    w_out = [
        rdma(a, b, w_send.at[i], w_recv.at[i], exp=partner) for i, (a, b) in enumerate(w_out)
    ]
    for copy in w_own + w_out:
        copy.start()

    own.wait()

    @pl.loop(1, NE)
    def _(d):
        frm = lax.rem(e + d, NE)
        rs_copy(attn_ref, parts, rs_send, rs_recv, frm, frm).wait_recv()

    def summed(buf):
        acc = buf[0].astype(F32)
        for i in range(1, NE):
            acc += buf[i].astype(F32)
        return acc

    mixed_share = (resid_ref[...].astype(F32) + summed(parts)).astype(BF)
    mixed[...] = mixed_share
    wide = mixed_share.astype(F32)
    scale = lax.rsqrt(jnp.mean(wide * wide, axis=-1, keepdims=True) + 1e-05)
    normed[exp_block(e), :] = (wide * scale * gain_ref[...]).astype(BF)

    def ag_copy(buf, send, recv, to, frm):
        return rdma(buf.at[exp_block(frm)], buf.at[exp_block(frm)], send.at[to], recv.at[frm], exp=to)

    @pl.loop(1, NE)
    def _(d):
        to = lax.rem(e + d, NE)
        ag_copy(normed, ag_send, ag_recv, to, e).start()

    @pl.loop(1, NE)
    def _(d):
        frm = lax.rem(e + d, NE)
        ag_copy(normed, ag_send, ag_recv, frm, frm).wait_recv()

    def di_copy(to, frm):
        return rdma(packed.at[to], arrived.at[frm], di_send.at[to], di_recv.at[frm], seq=to)

    def self_copy():
        return pltpu.make_async_copy(packed.at[s], arrived.at[s], own_sem.at[1])

    for d in (2, 1, 3, 0):
        q = lax.rem(quad + d, NS // QUAD)
        block = jnp.dot(pick_ref[q], normed[...], preferred_element_type=F32).astype(BF)
        for j in range(QUAD):
            packed[q * QUAD + j] = block[j * SLOTS : (j + 1) * SLOTS]
        if d:
            for j in range(QUAD):
                di_copy(q * QUAD + j, s).start()
        else:
            for j in range(1, QUAD):
                di_copy(quad * QUAD + lax.rem(s + j, QUAD), s).start()
            self_copy().start()

    for copy in w_own:
        copy.wait()
    for copy in w_out:
        copy.wait_recv()

    def re_copy(to, frm):
        return rdma(outgoing.at[to], returned.at[frm], re_send.at[to], re_recv.at[frm], seq=to)

    def self_back():
        return pltpu.make_async_copy(outgoing.at[s], returned.at[s], own_sem.at[2])

    def activated(acc):
        gate = jnp.minimum(acc[:, : 2 * hid], 7.0)
        up = jnp.clip(acc[:, 2 * hid :], -7.0, 7.0)
        return (up + 1.0) * gate * jax.nn.sigmoid(1.702 * gate)

    for d in (0, 1, 3, 2):
        q = lax.rem(quad + d, NS // QUAD)
        if d:
            for j in range(QUAD):
                di_copy(q * QUAD + j, q * QUAD + j).wait_recv()
        else:
            for j in range(1, QUAD):
                frm = quad * QUAD + lax.rem(s + j, QUAD)
                di_copy(frm, frm).wait_recv()
            self_copy().wait()
        x = jnp.concatenate([arrived[q * QUAD + j] for j in range(QUAD)], 0)
        acc = jnp.dot(x, w_in[...], preferred_element_type=F32)
        slot = lax.rem(lax.broadcasted_iota(jnp.int32, (QUAD * SLOTS, 2 * hid), 0), SLOTS)
        first = jnp.where(slot < CAP, activated(acc[:, : 4 * hid]), 0.0)
        second = jnp.where(slot >= CAP, activated(acc[:, 4 * hid :]), 0.0)
        hidden = jnp.concatenate([first, second], 1).astype(BF)
        block = jnp.dot(hidden, w_down[...], preferred_element_type=F32).astype(BF)
        for j in range(QUAD):
            outgoing[q * QUAD + j] = block[j * SLOTS : (j + 1) * SLOTS]
        if d:
            for j in range(QUAD):
                re_copy(q * QUAD + j, s).start()
        else:
            for j in range(1, QUAD):
                re_copy(quad * QUAD + lax.rem(s + j, QUAD), s).start()
            self_back().start()

    for n, d in enumerate((0, 1, 3, 2)):
        q = lax.rem(quad + d, NS // QUAD)
        if d:
            for j in range(QUAD):
                re_copy(q * QUAD + j, q * QUAD + j).wait_recv()
        else:
            for j in range(1, QUAD):
                frm = quad * QUAD + lax.rem(s + j, QUAD)
                re_copy(frm, frm).wait_recv()
            self_back().wait()
        y = jnp.concatenate([returned[q * QUAD + j] for j in range(QUAD)], 0)
        add = jnp.dot(comb_ref[q], y, preferred_element_type=F32)
        if n == 0:
            total[...] = add
        elif n < 3:
            total[...] += add
        else:
            moe_part[...] = (total[...] + add).astype(BF)

    @pl.loop(1, NE)
    def _(d):
        to = lax.rem(e + d, NE)
        rs_copy(moe_part, parts2, rs2_send, rs2_recv, to, e).start()

    own2 = pltpu.make_async_copy(moe_part.at[exp_block(e)], parts2.at[e], own_sem.at[3])
    own2.start()
    own2.wait()

    @pl.loop(1, NE)
    def _(d):
        frm = lax.rem(e + d, NE)
        rs_copy(moe_part, parts2, rs2_send, rs2_recv, frm, frm).wait_recv()

    out_ref[exp_block(e), :] = (mixed[...].astype(F32) + summed(parts2)).astype(BF)

    @pl.loop(1, NE)
    def _(d):
        to = lax.rem(e + d, NE)
        ag_copy(out_ref, ag2_send, ag2_recv, to, e).start()

    @pl.loop(1, NE)
    def _(d):
        frm = lax.rem(e + d, NE)
        ag_copy(out_ref, ag2_send, ag2_recv, frm, frm).wait_recv()

    for copy in w_out:
        copy.wait_send()

    @pl.loop(1, NE)
    def _(d):
        to = lax.rem(e + d, NE)
        rs_copy(attn_ref, parts, rs_send, rs_recv, to, e).wait_send()
        ag_copy(normed, ag_send, ag_recv, to, e).wait_send()
        rs_copy(moe_part, parts2, rs2_send, rs2_recv, to, e).wait_send()
        ag_copy(out_ref, ag2_send, ag2_recv, to, e).wait_send()

    @pl.loop(1, NS)
    def _(d):
        to = lax.rem(s + d, NS)
        di_copy(to, s).wait_send()
        re_copy(to, s).wait_send()


def on_device(
    queries,
    key_rows,
    value_rows,
    sink_logits,
    residual,
    out_weight,
    norm_gain,
    expert_ids,
    route_gates,
    gate_proj,
    up_proj,
    down_proj,
):
    tok, width = residual.shape
    rows = tok // NE
    hid = down_proj.shape[1]
    column = lax.axis_index("exp")
    parity = (column // 2) % 2
    attn = attention(queries, key_rows, value_rows, sink_logits, out_weight)
    own_resid = lax.dynamic_slice_in_dim(residual, column * rows, rows, 0)
    pick, combine = routing(expert_ids, route_gates, parity)
    vmem = pl.BlockSpec(memory_space=pltpu.VMEM)
    hbm = pl.BlockSpec(memory_space=pl.ANY)
    dma = pltpu.SemaphoreType.DMA
    return pl.pallas_call(
        layer_kernel,
        out_shape=jax.ShapeDtypeStruct((tok, width), BF),
        in_specs=[vmem] * 5 + [hbm] * 3,
        out_specs=vmem,
        scratch_shapes=[
            pltpu.VMEM((NE, rows, width), BF),
            pltpu.VMEM((NE, rows, width), BF),
            pltpu.VMEM((tok, width), BF),
            pltpu.VMEM((rows, width), BF),
            pltpu.VMEM((NS, SLOTS, width), BF),
            pltpu.VMEM((NS, SLOTS, width), BF),
            pltpu.VMEM((NS, SLOTS, width), BF),
            pltpu.VMEM((NS, SLOTS, width), BF),
            pltpu.VMEM((width, 8 * hid), BF),
            pltpu.VMEM((4 * hid, width), BF),
            pltpu.VMEM((tok, width), F32),
            pltpu.VMEM((tok, width), BF),
            dma((6,)),
            dma((6,)),
            dma((6,)),
        ]
        + [dma((NE,))] * 12
        + [dma((4,))],
        compiler_params=pltpu.CompilerParams(
            collective_id=0, has_side_effects=True, vmem_limit_bytes=62 * 1024 * 1024
        ),
    )(attn, own_resid, norm_gain.reshape(1, width), pick, combine, gate_proj, up_proj, down_proj)


def solution(mesh):
    in_specs = (
        P("seq", "exp"),
        P("seq", None),
        P("seq", None),
        P("exp"),
        P("seq", None),
        P("exp", None),
        P(),
        P("seq", None),
        P("seq", None),
        P("seq", None, "exp"),
        P("seq", None, "exp"),
        P("seq", "exp", None),
    )
    return jax.shard_map(
        on_device, mesh=mesh, in_specs=in_specs, out_specs=P("seq", None), check_vma=False
    )
```

```python
import functools
import math

import jax
import jax.numpy as jnp
from jax import lax
from jax.experimental import pallas as pl
from jax.experimental.pallas import tpu as pltpu
from jax.sharding import PartitionSpec as P

HQ = 64
HK = 8
HEAD = 64
TOP = 4
WIN = 128
NS = 16
NE = 16
EXPERTS = 64
CAP = 24
SLOTS = 2 * CAP
QUAD = 4
NZ = 8
CUTS = (0, 768, 1536, 2304, 2880)
CHUNKS = tuple((a, b - a) for a, b in zip(CUTS, CUTS[1:]))
NC = len(CHUNKS)
NC_BOTH = 2
MESH = pl.DeviceIdType.MESH
BF = jnp.bfloat16
F32 = jnp.float32


def passed_along(x, axis, by):
    count = lax.axis_size(axis)
    pairs = [(i, i + by) for i in range(count) if 0 <= i + by < count]
    return lax.ppermute(x, axis, pairs)


def attention(queries, key_rows, value_rows, sink_logits, out_weight):
    tok_rows = queries.shape[0]
    local_heads = queries.shape[1] // HEAD
    per_group = HQ // HK
    column = lax.axis_index("exp")
    slab_index = lax.axis_index("seq")
    kv_start = column * local_heads // per_group
    key_own = lax.dynamic_slice_in_dim(key_rows, kv_start * HEAD, HEAD, 1)
    value_own = lax.dynamic_slice_in_dim(value_rows, kv_start * HEAD, HEAD, 1)
    both = jnp.concatenate([key_own, value_own], 1)
    tail = passed_along(both[tok_rows - WIN :], "seq", 1)
    full = jnp.concatenate([tail, both], 0)
    key_full, value_full = full[:, :HEAD], full[:, HEAD:]
    query_heads = queries.reshape(tok_rows, local_heads, HEAD)
    scores = jnp.einsum("qhd,kd->hqk", query_heads, key_full, preferred_element_type=F32) * (
        1.0 / math.sqrt(HEAD)
    )
    first_pos = slab_index * tok_rows
    q_pos = first_pos + jnp.arange(tok_rows, dtype=jnp.int32)
    k_pos = first_pos - WIN + jnp.arange(WIN + tok_rows, dtype=jnp.int32)
    allowed = (
        (k_pos[None, :] <= q_pos[:, None])
        & (k_pos[None, :] > q_pos[:, None] - WIN)
        & (k_pos[None, :] >= 0)
    )
    scores = jnp.where(allowed[None], scores, -1e30)
    row_top = jnp.maximum(jnp.max(scores, axis=-1), sink_logits[:, None])
    expo = jnp.exp(scores - row_top[..., None])
    denominator = jnp.sum(expo, axis=-1) + jnp.exp(sink_logits[:, None] - row_top)
    weights = (expo / denominator[..., None]).astype(BF)
    context = jnp.einsum("hqk,kd->qhd", weights, value_full, preferred_element_type=F32)
    context = context.astype(BF).reshape(tok_rows, local_heads * HEAD)
    return jnp.dot(context, out_weight, preferred_element_type=F32).astype(BF)


def routing(expert_ids, route_gates, parity):
    rows = expert_ids.shape[0]
    half = EXPERTS // 2
    ids = jnp.arange(half, dtype=jnp.int32)
    mine = (ids // 2) * 4 + 2 * parity + ids % 2
    hits = expert_ids[:, :, None] == mine[None, None, :]
    named = jnp.sum(hits.astype(F32), axis=1)
    gate_of = jnp.sum(jnp.where(hits, route_gates[:, :, None], 0.0), axis=1)
    earlier = (jnp.arange(rows)[:, None] > jnp.arange(rows)[None, :]).astype(BF)
    count = jnp.dot(earlier, named.astype(BF), preferred_element_type=F32)
    slot_of = jnp.where(named > 0, count, -1.0).astype(BF)
    columns = jnp.arange(half * CAP, dtype=jnp.int32)
    spread = (columns[None, :] // CAP == ids[:, None]).astype(BF)
    slot_wide = jnp.dot(slot_of, spread, preferred_element_type=F32)
    taken = slot_wide == (columns % CAP).astype(F32)[None, :]
    gate_wide = jnp.dot(gate_of.astype(BF), spread, preferred_element_type=F32)
    combine = jnp.where(taken, gate_wide, 0.0).astype(BF)
    pick = taken.astype(BF).T
    quad_cols = QUAD * SLOTS
    combine = combine.reshape(rows, -1, quad_cols).transpose(1, 0, 2)
    return pick.reshape(-1, quad_cols, rows), combine


def layer_kernel(
    attn_ref,
    resid_ref,
    gain_ref,
    pick_ref,
    comb_ref,
    gate_ref,
    up_ref,
    down_ref,
    out_ref,
    xin,
    zsrc,
    zin,
    zin2,
    pair,
    pair_in,
    normed,
    mixed,
    packed,
    arrived,
    outgoing,
    returned,
    w_in,
    w_down,
    acc,
    hidden,
    moe_part,
    result,
    w_local,
    w_send,
    w_recv,
    rx_send,
    rx_recv,
    rz_send,
    rz_recv,
    gx_send,
    gx_recv,
    gz_send,
    gz_recv,
    mx_send,
    mx_recv,
    di_send,
    di_recv,
    re_send,
    re_recv,
    own_sem,
):
    s = lax.axis_index("seq")
    e = lax.axis_index("exp")
    z = lax.div(e, 2)
    xh = lax.rem(e, 2)
    parity = lax.rem(z, 2)
    mate = e + 2 - 4 * parity
    across = e + 1 - 2 * xh
    rows = mixed.shape[1]
    quad = lax.div(s, QUAD)
    hid = gate_ref.shape[2]
    tok = NE * rows

    barrier = pltpu.get_barrier_semaphore()

    @pl.loop(1, NE)
    def _(d):
        pl.semaphore_signal(
            barrier, inc=1, device_id={"exp": lax.rem(e + d, NE)}, device_id_type=MESH
        )

    @pl.loop(1, NS)
    def _(d):
        pl.semaphore_signal(
            barrier, inc=1, device_id={"seq": lax.rem(s + d, NS)}, device_id_type=MESH
        )

    pl.semaphore_wait(barrier, NE + NS - 2)

    def rdma(src, dst, send, recv, **where):
        return pltpu.make_async_remote_copy(
            src_ref=src,
            dst_ref=dst,
            send_sem=send,
            recv_sem=recv,
            device_id=where,
            device_id_type=MESH,
        )

    def cols(c):
        return pl.ds(*CHUNKS[c])

    def other(d):
        return lax.rem(z + d, NZ)

    def rx(c):
        return rdma(
            attn_ref.at[:, 1 - xh, :, cols(c)],
            xin.at[:, :, cols(c)],
            rx_send.at[0, c],
            rx_recv.at[0, c],
            exp=across,
        )

    def rz(c, to, frm):
        return rdma(
            zsrc.at[to, :, cols(c)],
            zin.at[frm, :, cols(c)],
            rz_send.at[0, c],
            rz_recv.at[0, c],
            exp=2 * to + xh,
        )

    def rz_all(c):
        part = zin.at[pl.ds(0, NZ - 1), :, cols(c)]
        return rdma(part, part, rz_send.at[0, c], rz_recv.at[0, c], exp=across)

    def rx_done_rz_start(c):
        rx(c).wait_recv()
        both = attn_ref[:, xh, :, cols(c)].astype(F32) + xin[:, :, cols(c)].astype(F32)
        zsrc[:, :, cols(c)] = both.astype(BF)

        @pl.loop(1, NZ)
        def _(d):
            rz(c, other(NZ - d), z).start()

    def rz_sum(c):
        rz_all(c).wait_recv()
        sum_ = zsrc[z, :, cols(c)].astype(F32)
        for d in range(1, NZ):
            sum_ += zin[other(d), :, cols(c)].astype(F32)
        return sum_

    def ez(c, to, frm):
        return rdma(
            moe_part.at[to, :, :, cols(c)],
            zin2.at[frm, :, :, cols(c)],
            rz_send.at[1, c],
            rz_recv.at[1, c],
            exp=2 * to + xh,
        )

    def ez_all(c):
        part = zin2.at[pl.ds(0, NZ - 1), :, :, cols(c)]
        return rdma(part, part, rz_send.at[1, c], rz_recv.at[1, c], exp=across)

    def ez_start(c):
        @pl.loop(1, NZ)
        def _(d):
            ez(c, other(NZ - d), z).start()

    def ex(c):
        return rdma(
            pair.at[:, :, cols(c)],
            pair_in.at[:, :, cols(c)],
            rx_send.at[1, c],
            rx_recv.at[1, c],
            exp=across,
        )

    def ez_done_ex_start(c):
        ez_all(c).wait_recv()
        sum_ = moe_part[z, :, :, cols(c)].astype(F32)
        for d in range(1, NZ):
            sum_ += zin2[other(d), :, :, cols(c)].astype(F32)
        pair[:, :, cols(c)] = sum_.astype(BF)
        ex(c).start()

    def mixed_across(half):
        return rdma(mixed.at[half], mixed.at[half], mx_send.at[0], mx_recv.at[0], exp=across)

    def gz(n, c, to, frm):
        if n == 1 and c < NC_BOTH:
            block = result.at[frm, :, :, cols(c)]
        else:
            block = (normed, result)[n].at[frm, xh, :, cols(c)]
        return rdma(block, block, gz_send.at[n, c], gz_recv.at[n, c], exp=2 * to + xh)

    def gz_start(n, c):
        @pl.loop(1, NZ)
        def _(d):
            gz(n, c, other(NZ - d), z).start()

    def gz_all(n, c):
        if n == 1 and c < NC_BOTH:
            part = result.at[pl.ds(0, NZ - 1), :, :, cols(c)]
        else:
            part = (normed, result)[n].at[pl.ds(0, NZ - 1), xh, :, cols(c)]
        return rdma(part, part, gz_send.at[n, c], gz_recv.at[n, c], exp=across)

    def gz_wait(n, c):
        gz_all(n, c).wait_recv()

    def gx(n, c, half):
        buf = (normed, result)[n]
        block = buf.at[:, half, :, cols(c)]
        return rdma(block, block, gx_send.at[n, c], gx_recv.at[n, c], exp=across)

    def gz_done_gx_start(n, c):
        gz_wait(n, c)
        gx(n, c, xh).start()

    def weight_pairs(c):
        keep, give = [], []
        for ref in (gate_ref, up_ref, down_ref):
            for k in range(2):
                at = (0, 2 * hid, 0)[len(keep) // 2] + k * (2 if ref is down_ref else 4) * hid
                buf = w_down if ref is down_ref else w_in
                keep.append((ref.at[2 * parity + k, cols(c)], buf.at[cols(c), pl.ds(at, hid)]))
                give.append(
                    (ref.at[2 - 2 * parity + k, cols(c)], buf.at[cols(c), pl.ds(at + hid, hid)])
                )
        keep = [pltpu.make_async_copy(a, b, w_local.at[c, i]) for i, (a, b) in enumerate(keep)]
        give = [
            rdma(a, b, w_send.at[c, i], w_recv.at[c, i], exp=mate) for i, (a, b) in enumerate(give)
        ]
        return keep, give

    weights = [weight_pairs(c) for c in range(NC)]

    queue = [copy for c in range(NC) for copy in weights[c][1][:4]]
    queue += [copy for c in range(NC) for copy in weights[c][1][4:]]

    def give(count):
        for copy in queue[:count]:
            copy.start()
        del queue[:count]

    for c in range(NC):
        rx(c).start()
    give(2)
    for c in range(NC):
        for copy in weights[c][0]:
            copy.start()
    for c in range(NC):
        rx_done_rz_start(c)
    pick_own = (
        lax.broadcasted_iota(jnp.int32, (rows, tok), 1)
        == e * rows + lax.broadcasted_iota(jnp.int32, (rows, tok), 0)
    ).astype(BF)
    square = jnp.zeros((rows, 1), F32)
    for c in range(NC):
        own = lax.dot_general(
            pick_own,
            resid_ref[cols(c), :],
            (((1,), (1,)), ((), ())),
            preferred_element_type=F32,
        )
        mine = (own + rz_sum(c)).astype(BF)
        mixed[xh, :, cols(c)] = mine
        wide = mine.astype(F32)
        square += jnp.sum(wide * wide, axis=-1, keepdims=True)
    scale = lax.rsqrt(square / mixed.shape[2] + 1e-05)
    for c in range(NC):
        wide = mixed[xh, :, cols(c)].astype(F32)
        normed[z, xh, :, cols(c)] = (wide * scale * gain_ref[:, cols(c)]).astype(BF)
        gz_start(0, c)
    mixed_across(xh).start()
    give(len(queue))

    def di(c, to, frm, d=0):
        return rdma(
            packed.at[to, :, cols(c)],
            arrived.at[frm, :, cols(c)],
            di_send.at[c],
            di_recv.at[c, d],
            seq=to,
        )

    def di_own(c):
        return pltpu.make_async_copy(
            packed.at[s, :, cols(c)], arrived.at[s, :, cols(c)], own_sem.at[0, c]
        )

    def re(c, to, frm, d=0):
        return rdma(
            outgoing.at[to, :, cols(c)],
            returned.at[frm, :, cols(c)],
            re_send.at[c],
            re_recv.at[c, d],
            seq=to,
        )

    def re_own(c):
        return pltpu.make_async_copy(
            outgoing.at[s, :, cols(c)], returned.at[s, :, cols(c)], own_sem.at[1, c]
        )

    def peers(d):
        if d:
            q = lax.rem(quad + d, NS // QUAD)
            return [q * QUAD + j for j in range(QUAD)]
        return [quad * QUAD + lax.rem(s + j, QUAD) for j in range(1, QUAD)]

    def put(buf, q, c, block):
        for j in range(QUAD):
            buf[q * QUAD + j, :, cols(c)] = block[j * SLOTS : (j + 1) * SLOTS]

    def start(copy, own, d, c):
        for to in peers(d):
            copy(c, to, s, (NS // QUAD - d) % (NS // QUAD)).start()
        if d == 0:
            own(c).start()

    def group(copy, c, d, count):
        buf = arrived if copy is di else returned
        part = buf.at[pl.ds(0, count), :, cols(c)]
        send, recv = (di_send, di_recv) if copy is di else (re_send, re_recv)
        return rdma(part, part, send.at[c], recv.at[c, d], exp=across)

    def wait(copy, own, d, c):
        group(copy, c, d, QUAD if d else QUAD - 1).wait_recv()
        if d == 0:
            own(c).wait()

    def pack(c):
        gx(0, c, 1 - xh).wait_recv()
        full = normed[:, :, :, cols(c)].reshape(tok, CHUNKS[c][1])
        for d in (2, 1, 3, 0):
            q = lax.rem(quad + d, NS // QUAD)
            put(packed, q, c, jnp.dot(pick_ref[q], full, preferred_element_type=F32).astype(BF))
            start(di, di_own, d, c)

    for c in range(NC):
        gz_done_gx_start(0, c)
    for c in range(NC):
        pack(c)

    for c in range(NC):
        for copy in weights[c][0]:
            copy.wait()
        for copy in weights[c][1][:4]:
            copy.wait_recv()
        for d in (0, 1, 3, 2):
            q = lax.rem(quad + d, NS // QUAD)
            wait(di, di_own, d, c)
            x = jnp.concatenate([arrived[q * QUAD + j, :, cols(c)] for j in range(QUAD)], 0)
            add = jnp.dot(x, w_in[cols(c), :], preferred_element_type=F32)
            if c:
                acc[q] += add
            else:
                acc[q] = add

    def activated(block):
        gate = jnp.minimum(block[:, : 2 * hid], 7.0)
        up = jnp.clip(block[:, 2 * hid :], -7.0, 7.0)
        return (up + 1.0) * gate * jax.nn.sigmoid(1.702 * gate)

    slot = lax.rem(lax.broadcasted_iota(jnp.int32, (QUAD * SLOTS, 2 * hid), 0), SLOTS)
    for q in range(NS // QUAD):
        first = jnp.where(slot < CAP, activated(acc[q, :, : 4 * hid]), 0.0)
        second = jnp.where(slot >= CAP, activated(acc[q, :, 4 * hid :]), 0.0)
        hidden[q] = jnp.concatenate([first, second], 1).astype(BF)

    def give_back(c):
        for copy in weights[c][1][4:]:
            copy.wait_recv()
        for d in (2, 1, 3, 0):
            q = lax.rem(quad + d, NS // QUAD)
            block = lax.dot_general(
                hidden[q],
                w_down[cols(c), :],
                (((1,), (1,)), ((), ())),
                preferred_element_type=F32,
            )
            put(outgoing, q, c, block.astype(BF))
            start(re, re_own, d, c)

    def combine(c):
        sum_ = None
        for d in (0, 1, 3, 2):
            q = lax.rem(quad + d, NS // QUAD)
            wait(re, re_own, d, c)
            y = jnp.concatenate([returned[q * QUAD + j, :, cols(c)] for j in range(QUAD)], 0)
            add = jnp.dot(comb_ref[q], y, preferred_element_type=F32)
            sum_ = add if sum_ is None else sum_ + add
        moe_part[:, :, :, cols(c)] = sum_.astype(BF).reshape(NZ, 2, rows, CHUNKS[c][1])
        ez_start(c)

    def finish_rows(c):
        ex(c).wait_recv()
        mine = slice(None) if c < NC_BOTH else xh
        both = pair[mine, :, cols(c)].astype(F32) + pair_in[mine, :, cols(c)].astype(F32)
        done = mixed[mine, :, cols(c)].astype(F32) + both
        result[z, mine, :, cols(c)] = done.astype(BF)
        gz_start(1, c)

    def write_out(c):
        if c < NC_BOTH:
            gz_wait(1, c)
        else:
            gx(1, c, 1 - xh).wait_recv()
        out_ref[cols(c), :] = result[:, :, :, cols(c)].reshape(tok, CHUNKS[c][1]).T

    give_back(0)
    give_back(1)
    mixed_across(1 - xh).wait_recv()
    for c in range(NC):
        combine(c)
        if c:
            finish_rows(c - 1)
        ez_done_ex_start(c)
        if c + 2 < NC:
            give_back(c + 2)
    finish_rows(NC - 1)
    for c in range(NC):
        if c >= NC_BOTH:
            gz_done_gx_start(1, c)
        else:
            write_out(c)
    for c in range(NC_BOTH, NC):
        write_out(c)

    mixed_across(xh).wait_send()
    for c in range(NC):
        for copy in weights[c][1]:
            copy.wait_send()
        rx(c).wait_send()
        ex(c).wait_send()
        gx(0, c, xh).wait_send()
        if c >= NC_BOTH:
            gx(1, c, xh).wait_send()

        rz_all(c).wait_send()
        ez_all(c).wait_send()
        gz_all(0, c).wait_send()
        gz_all(1, c).wait_send()
        group(di, c, 0, NS - 1).wait_send()
        group(re, c, 0, NS - 1).wait_send()


def on_device(
    queries,
    key_rows,
    value_rows,
    sink_logits,
    residual,
    out_weight,
    norm_gain,
    expert_ids,
    route_gates,
    gate_proj,
    up_proj,
    down_proj,
):
    tok, width = residual.shape
    rows = tok // NE
    hid = down_proj.shape[1]
    column = lax.axis_index("exp")
    parity = (column // 2) % 2
    attn = attention(queries, key_rows, value_rows, sink_logits, out_weight)
    pick, combine = routing(expert_ids, route_gates, parity)
    vmem = pl.BlockSpec(memory_space=pltpu.VMEM)
    hbm = pl.BlockSpec(memory_space=pl.ANY)
    dma = pltpu.SemaphoreType.DMA
    sums = [pltpu.VMEM((NZ, rows, width), BF)] * 3
    slots = pltpu.VMEM((NS, SLOTS, width), BF)
    whole = pltpu.VMEM((NZ, 2, rows, width), BF)
    both = pltpu.VMEM((2, rows, width), BF)
    out = pl.pallas_call(
        layer_kernel,
        out_shape=jax.ShapeDtypeStruct((width, tok), BF),
        in_specs=[vmem] * 5 + [hbm] * 3,
        out_specs=vmem,
        scratch_shapes=sums
        + [whole, both, both]
        + [
            whole,
            both,
            slots,
            slots,
            slots,
            slots,
            pltpu.VMEM((width, 8 * hid), BF),
            pltpu.VMEM((width, 4 * hid), BF),
            pltpu.VMEM((NS // QUAD, QUAD * SLOTS, 8 * hid), F32),
            pltpu.VMEM((NS // QUAD, QUAD * SLOTS, 4 * hid), BF),
            whole,
            whole,
        ]
        + [dma((NC, 6))] * 3
        + [dma((2, NC))] * 8
        + [dma((1,))] * 2
        + [dma((NC,)), dma((NC, NS // QUAD))] * 2
        + [dma((2, NC))],
        compiler_params=pltpu.CompilerParams(
            collective_id=0, has_side_effects=True, vmem_limit_bytes=62 * 1024 * 1024
        ),
    )(
        attn.reshape(NZ, 2, rows, width),
        residual.T,
        norm_gain.reshape(1, width),
        pick,
        combine,
        gate_proj,
        up_proj,
        down_proj.transpose(0, 2, 1),
    )
    return out.T


def solution(mesh):
    in_specs = (
        P("seq", "exp"),
        P("seq", None),
        P("seq", None),
        P("exp"),
        P("seq", None),
        P("exp", None),
        P(),
        P("seq", None),
        P("seq", None),
        P("seq", None, "exp"),
        P("seq", None, "exp"),
        P("seq", "exp", None),
    )
    return jax.shard_map(
        on_device, mesh=mesh, in_specs=in_specs, out_specs=P("seq", None), check_vma=False
    )
```

```python
import functools
import math

import jax
import jax.numpy as jnp
from jax import lax
from jax.experimental import pallas as pl
from jax.experimental.pallas import tpu as pltpu
from jax.sharding import PartitionSpec as P

HQ = 64
HK = 8
HEAD = 64
TOP = 4
WIN = 128
NS = 16
NE = 16
EXPERTS = 64
CAP = 24
SLOTS = 2 * CAP
QUAD = 4
NZ = 8
CUTS = (0, 768, 1536, 2304, 2880)
CHUNKS = tuple((a, b - a) for a, b in zip(CUTS, CUTS[1:]))
NC = len(CHUNKS)
NC_BOTH = 2
MESH = pl.DeviceIdType.MESH
BF = jnp.bfloat16
F32 = jnp.float32


def layer_kernel(
    query_ref,
    sink_ref,
    gain_ref,
    ids_ref,
    gates_ref,
    key_ref,
    value_ref,
    proj_ref,
    skip_ref,
    gate_ref,
    up_ref,
    down_ref,
    out_ref,
    keys,
    values,
    proj,
    resid,
    pick,
    comb,
    attn,
    xin,
    zsrc,
    zin,
    zin2,
    pair,
    pair_in,
    normed,
    mixed,
    packed,
    arrived,
    outgoing,
    returned,
    w_in,
    w_down,
    acc,
    hidden,
    moe_part,
    result,
    w_local,
    w_send,
    w_recv,
    rx_send,
    rx_recv,
    rz_send,
    rz_recv,
    gx_send,
    gx_recv,
    gz_send,
    gz_recv,
    mx_send,
    mx_recv,
    di_send,
    di_recv,
    re_send,
    re_recv,
    own_sem,
    load_sem,
    halo_send,
    halo_recv,
):
    s = lax.axis_index("seq")
    e = lax.axis_index("exp")
    z = lax.div(e, 2)
    xh = lax.rem(e, 2)
    parity = lax.rem(z + s, 2)
    mate = 2 * lax.rem(z + 1 + (NZ - 2) * parity, NZ) + xh
    across = e + 1 - 2 * xh
    rows = mixed.shape[1]
    quad = lax.div(s, QUAD)
    hid = gate_ref.shape[2]
    tok = NE * rows

    lanes = pl.ds(pl.multiple_of(lax.div(e, 4) * 2 * HEAD, 2 * HEAD), 2 * HEAD)
    loads = [
        pltpu.make_async_copy(src, dst, load_sem.at[i])
        for i, (src, dst) in enumerate(
            (
                (key_ref.at[:, lanes], keys.at[pl.ds(WIN, tok)]),
                (value_ref.at[:, lanes], values.at[pl.ds(WIN, tok)]),
                (proj_ref, proj),
                (skip_ref, resid),
            )
        )
    ]
    for copy in loads:
        copy.start()

    barrier = pltpu.get_barrier_semaphore()

    @pl.loop(1, NE)
    def _(d):
        pl.semaphore_signal(
            barrier, inc=1, device_id={"exp": lax.rem(e + d, NE)}, device_id_type=MESH
        )

    @pl.loop(1, NS)
    def _(d):
        pl.semaphore_signal(
            barrier, inc=1, device_id={"seq": lax.rem(s + d, NS)}, device_id_type=MESH
        )

    def head_of(buf, at):
        both = buf[pl.ds(at, 2 * WIN), :]
        return jnp.where(lax.rem(lax.div(e, 2), 2) == 1, both[:, HEAD:], both[:, :HEAD])

    def context(half):
        heads = query_ref.shape[1] // HEAD
        at = half * WIN
        query = jnp.concatenate(
            [query_ref[at : at + WIN, h * HEAD : (h + 1) * HEAD] for h in range(heads)], 0
        )
        scores = lax.dot_general(
            query, head_of(keys, at), (((1,), (1,)), ((), ())), preferred_element_type=F32
        ) * (1.0 / math.sqrt(HEAD))
        row = lax.rem(lax.broadcasted_iota(jnp.int32, scores.shape, 0), WIN)
        col = lax.broadcasted_iota(jnp.int32, scores.shape, 1)
        allowed = (col > row) & (col <= row + WIN)
        if half == 0:
            allowed = allowed & ((col >= WIN) | (s > 0))
        scores = jnp.where(allowed, scores, -1e30)
        sink = jnp.concatenate(
            [jnp.broadcast_to(sink_ref[:, h : h + 1], (WIN, 1)) for h in range(heads)], 0
        )
        top = jnp.maximum(jnp.max(scores, axis=-1, keepdims=True), sink)
        expo = jnp.exp(scores - top)
        total = jnp.sum(expo, axis=-1, keepdims=True) + jnp.exp(sink - top)
        weights = (expo / total).astype(BF)
        out = jnp.dot(weights, head_of(values, at), preferred_element_type=F32).astype(BF)
        return jnp.concatenate([out[h * WIN : (h + 1) * WIN] for h in range(heads)], 1)

    loads[0].wait()
    loads[1].wait()
    second = context(1)
    pl.semaphore_wait(barrier, NE + NS - 2)

    def rdma(src, dst, send, recv, **where):
        return pltpu.make_async_remote_copy(
            src_ref=src,
            dst_ref=dst,
            send_sem=send,
            recv_sem=recv,
            device_id=where,
            device_id_type=MESH,
        )

    def cols(c):
        return pl.ds(*CHUNKS[c])

    def other(d):
        return lax.rem(z + d, NZ)

    def rx(c):
        return rdma(
            attn.at[:, 1 - xh, :, cols(c)],
            xin.at[:, :, cols(c)],
            rx_send.at[0, c],
            rx_recv.at[0, c],
            exp=across,
        )

    def rz(c, to, frm):
        return rdma(
            zsrc.at[to, :, cols(c)],
            zin.at[frm, :, cols(c)],
            rz_send.at[0, c],
            rz_recv.at[0, c],
            exp=2 * to + xh,
        )

    def rz_all(c):
        part = zin.at[pl.ds(0, NZ - 1), :, cols(c)]
        return rdma(part, part, rz_send.at[0, c], rz_recv.at[0, c], exp=across)

    def rx_done_rz_start(c):
        rx(c).wait_recv()
        both = attn[:, xh, :, cols(c)].astype(F32) + xin[:, :, cols(c)].astype(F32)
        zsrc[:, :, cols(c)] = both.astype(BF)

        @pl.loop(1, NZ)
        def _(d):
            rz(c, other(NZ - d), z).start()

    def rz_sum(c):
        rz_all(c).wait_recv()
        sum_ = zsrc[z, :, cols(c)].astype(F32)
        for d in range(1, NZ):
            sum_ += zin[other(d), :, cols(c)].astype(F32)
        return sum_

    def ez(c, to, frm):
        return rdma(
            moe_part.at[to, :, :, cols(c)],
            zin2.at[frm, :, :, cols(c)],
            rz_send.at[1, c],
            rz_recv.at[1, c],
            exp=2 * to + xh,
        )

    def ez_all(c):
        part = zin2.at[pl.ds(0, NZ - 1), :, :, cols(c)]
        return rdma(part, part, rz_send.at[1, c], rz_recv.at[1, c], exp=across)

    def ez_start(c):
        @pl.loop(1, NZ)
        def _(d):
            ez(c, other(NZ - d), z).start()

    def ex(c):
        return rdma(
            pair.at[:, :, cols(c)],
            pair_in.at[:, :, cols(c)],
            rx_send.at[1, c],
            rx_recv.at[1, c],
            exp=across,
        )

    def ez_done_ex_start(c):
        ez_all(c).wait_recv()
        sum_ = moe_part[z, :, :, cols(c)].astype(F32)
        for d in range(1, NZ):
            sum_ += zin2[other(d), :, :, cols(c)].astype(F32)
        pair[:, :, cols(c)] = sum_.astype(BF)
        ex(c).start()

    def mixed_across(half):
        return rdma(mixed.at[half], mixed.at[half], mx_send.at[0], mx_recv.at[0], exp=across)

    def gz(n, c, to, frm):
        if n == 1 and c < NC_BOTH:
            block = result.at[frm, :, :, cols(c)]
        else:
            block = (normed, result)[n].at[frm, xh, :, cols(c)]
        return rdma(block, block, gz_send.at[n, c], gz_recv.at[n, c], exp=2 * to + xh)

    def gz_start(n, c):
        @pl.loop(1, NZ)
        def _(d):
            gz(n, c, other(NZ - d), z).start()

    def gz_all(n, c):
        if n == 1 and c < NC_BOTH:
            part = result.at[pl.ds(0, NZ - 1), :, :, cols(c)]
        else:
            part = (normed, result)[n].at[pl.ds(0, NZ - 1), xh, :, cols(c)]
        return rdma(part, part, gz_send.at[n, c], gz_recv.at[n, c], exp=across)

    def gz_wait(n, c):
        gz_all(n, c).wait_recv()

    def gx(n, c, half):
        buf = (normed, result)[n]
        block = buf.at[:, half, :, cols(c)]
        return rdma(block, block, gx_send.at[n, c], gx_recv.at[n, c], exp=across)

    def gz_done_gx_start(n, c):
        gz_wait(n, c)
        gx(n, c, xh).start()

    def weight_pairs(c):
        keep, give = [], []
        for ref in (gate_ref, up_ref, down_ref):
            for k in range(2):
                at = (0, 2 * hid, 0)[len(keep) // 2] + k * (2 if ref is down_ref else 4) * hid
                buf = w_down if ref is down_ref else w_in
                keep.append((ref.at[2 * parity + k, cols(c)], buf.at[cols(c), pl.ds(at, hid)]))
                give.append(
                    (ref.at[2 - 2 * parity + k, cols(c)], buf.at[cols(c), pl.ds(at + hid, hid)])
                )
        keep = [pltpu.make_async_copy(a, b, w_local.at[c, i]) for i, (a, b) in enumerate(keep)]
        give = [
            rdma(a, b, w_send.at[c, i], w_recv.at[c, i], exp=mate) for i, (a, b) in enumerate(give)
        ]
        return keep, give

    weights = [weight_pairs(c) for c in range(NC)]

    queue = [copy for c in range(NC) for copy in weights[c][1][:4]]
    queue += [copy for c in range(NC) for copy in weights[c][1][4:]]

    def give(count):
        for copy in queue[:count]:
            copy.start()
        del queue[:count]

    halo = [
        rdma(
            ref.at[pl.ds(tok - WIN, WIN), lanes],
            buf.at[pl.ds(0, WIN)],
            halo_send.at[i],
            halo_recv.at[i],
            seq=lax.rem(s + 1, NS),
        )
        for i, (ref, buf) in enumerate(((key_ref, keys), (value_ref, values)))
    ]
    for copy in halo:
        copy.start()
    give(4)
    for c in range(NC):
        for copy in weights[c][0]:
            copy.start()
    loads[2].wait()
    for copy in halo:
        copy.wait_recv()
    mixed_heads = jnp.concatenate([context(0), second], 0)
    for c in range(NC):
        part = lax.dot_general(
            mixed_heads, proj[cols(c), :], (((1,), (1,)), ((), ())), preferred_element_type=F32
        )
        attn[:, :, :, cols(c)] = part.astype(BF).reshape(NZ, 2, rows, CHUNKS[c][1])
        rx(c).start()

    half = EXPERTS // 2
    index = lax.broadcasted_iota(jnp.int32, (half, tok), 0)
    group_of = lax.div(index, 2)
    mine = 4 * group_of + 2 * lax.rem(group_of + z, 2) + lax.rem(index, 2)
    named = jnp.zeros((half, tok), F32)
    gate_of = jnp.zeros((half, tok), F32)
    for k in range(TOP):
        hit = ids_ref[k : k + 1, :] == mine
        named += jnp.where(hit, 1.0, 0.0)
        gate_of += jnp.where(hit, gates_ref[k : k + 1, :], 0.0)
    earlier = lax.broadcasted_iota(jnp.int32, (tok, tok), 0) < lax.broadcasted_iota(
        jnp.int32, (tok, tok), 1
    )
    count = jnp.dot(
        named.astype(BF), jnp.where(earlier, 1.0, 0.0).astype(BF), preferred_element_type=F32
    )
    slot_of = jnp.where(named > 0.0, count, -1.0).astype(BF)
    gate_of = gate_of.astype(BF)
    for q in range(NS // QUAD):
        shape = (QUAD * SLOTS, half)
        place = lax.div(lax.broadcasted_iota(jnp.int32, shape, 0), CAP) + q * 2 * QUAD
        spread = jnp.where(place == lax.broadcasted_iota(jnp.int32, shape, 1), 1.0, 0.0)
        spread = spread.astype(BF)
        wide = jnp.dot(spread, slot_of, preferred_element_type=F32)
        number = lax.rem(lax.broadcasted_iota(jnp.int32, (QUAD * SLOTS, tok), 0), CAP)
        taken = wide == number.astype(F32)
        gate_wide = jnp.dot(spread, gate_of, preferred_element_type=F32)
        pick[q] = jnp.where(taken, 1.0, 0.0).astype(BF)
        comb[q] = jnp.where(taken, gate_wide, 0.0).T.astype(BF)
    loads[3].wait()

    for c in range(NC):
        rx_done_rz_start(c)
    pick_own = (
        lax.broadcasted_iota(jnp.int32, (rows, tok), 1)
        == e * rows + lax.broadcasted_iota(jnp.int32, (rows, tok), 0)
    ).astype(BF)
    square = jnp.zeros((rows, 1), F32)
    for c in range(NC):
        own = lax.dot_general(
            pick_own,
            resid[cols(c), :],
            (((1,), (1,)), ((), ())),
            preferred_element_type=F32,
        )
        mine = (own + rz_sum(c)).astype(BF)
        mixed[xh, :, cols(c)] = mine
        wide = mine.astype(F32)
        square += jnp.sum(wide * wide, axis=-1, keepdims=True)
    scale = lax.rsqrt(square / mixed.shape[2] + 1e-05)
    for c in range(NC):
        wide = mixed[xh, :, cols(c)].astype(F32)
        normed[z, xh, :, cols(c)] = (wide * scale * gain_ref[:, cols(c)]).astype(BF)
        gz_start(0, c)
    mixed_across(xh).start()
    give(len(queue))

    def di(c, to, frm, d=0):
        return rdma(
            packed.at[to, :, cols(c)],
            arrived.at[frm, :, cols(c)],
            di_send.at[c],
            di_recv.at[c, d],
            seq=to,
        )

    def di_own(c):
        return pltpu.make_async_copy(
            packed.at[s, :, cols(c)], arrived.at[s, :, cols(c)], own_sem.at[0, c]
        )

    def re(c, to, frm, d=0):
        return rdma(
            outgoing.at[to, :, cols(c)],
            returned.at[frm, :, cols(c)],
            re_send.at[c],
            re_recv.at[c, d],
            seq=to,
        )

    def re_own(c):
        return pltpu.make_async_copy(
            outgoing.at[s, :, cols(c)], returned.at[s, :, cols(c)], own_sem.at[1, c]
        )

    def peers(d):
        if d:
            q = lax.rem(quad + d, NS // QUAD)
            return [q * QUAD + j for j in range(QUAD)]
        return [quad * QUAD + lax.rem(s + j, QUAD) for j in range(1, QUAD)]

    def put(buf, q, c, block):
        for j in range(QUAD):
            buf[q * QUAD + j, :, cols(c)] = block[j * SLOTS : (j + 1) * SLOTS]

    def start(copy, own, d, c):
        for to in peers(d):
            copy(c, to, s, (NS // QUAD - d) % (NS // QUAD)).start()
        if d == 0:
            own(c).start()

    def group(copy, c, d, count):
        buf = arrived if copy is di else returned
        part = buf.at[pl.ds(0, count), :, cols(c)]
        send, recv = (di_send, di_recv) if copy is di else (re_send, re_recv)
        return rdma(part, part, send.at[c], recv.at[c, d], exp=across)

    def wait(copy, own, d, c):
        group(copy, c, d, QUAD if d else QUAD - 1).wait_recv()
        if d == 0:
            own(c).wait()

    def pack(c):
        gx(0, c, 1 - xh).wait_recv()
        full = normed[:, :, :, cols(c)].reshape(tok, CHUNKS[c][1])
        for d in (2, 1, 3, 0):
            q = lax.rem(quad + d, NS // QUAD)
            put(packed, q, c, jnp.dot(pick[q], full, preferred_element_type=F32).astype(BF))
            start(di, di_own, d, c)

    for c in range(NC):
        gz_done_gx_start(0, c)
    for c in range(NC):
        pack(c)

    for c in range(NC):
        for copy in weights[c][0]:
            copy.wait()
        for copy in weights[c][1][:4]:
            copy.wait_recv()
        for d in (0, 1, 3, 2):
            q = lax.rem(quad + d, NS // QUAD)
            wait(di, di_own, d, c)
            x = jnp.concatenate([arrived[q * QUAD + j, :, cols(c)] for j in range(QUAD)], 0)
            add = jnp.dot(x, w_in[cols(c), :], preferred_element_type=F32)
            if c:
                acc[q] += add
            else:
                acc[q] = add

    def activated(block):
        gate = jnp.minimum(block[:, : 2 * hid], 7.0)
        up = jnp.clip(block[:, 2 * hid :], -7.0, 7.0)
        return (up + 1.0) * gate * jax.nn.sigmoid(1.702 * gate)

    slot = lax.rem(lax.broadcasted_iota(jnp.int32, (QUAD * SLOTS, 2 * hid), 0), SLOTS)
    for q in range(NS // QUAD):
        first = jnp.where(slot < CAP, activated(acc[q, :, : 4 * hid]), 0.0)
        second = jnp.where(slot >= CAP, activated(acc[q, :, 4 * hid :]), 0.0)
        hidden[q] = jnp.concatenate([first, second], 1).astype(BF)

    def give_back(c):
        for copy in weights[c][1][4:]:
            copy.wait_recv()
        for d in (2, 1, 3, 0):
            q = lax.rem(quad + d, NS // QUAD)
            block = lax.dot_general(
                hidden[q],
                w_down[cols(c), :],
                (((1,), (1,)), ((), ())),
                preferred_element_type=F32,
            )
            put(outgoing, q, c, block.astype(BF))
            start(re, re_own, d, c)

    def combine(c):
        sum_ = None
        for d in (0, 1, 3, 2):
            q = lax.rem(quad + d, NS // QUAD)
            wait(re, re_own, d, c)
            y = jnp.concatenate([returned[q * QUAD + j, :, cols(c)] for j in range(QUAD)], 0)
            add = jnp.dot(comb[q], y, preferred_element_type=F32)
            sum_ = add if sum_ is None else sum_ + add
        moe_part[:, :, :, cols(c)] = sum_.astype(BF).reshape(NZ, 2, rows, CHUNKS[c][1])
        ez_start(c)

    def finish_rows(c):
        ex(c).wait_recv()
        mine = slice(None) if c < NC_BOTH else xh
        both = pair[mine, :, cols(c)].astype(F32) + pair_in[mine, :, cols(c)].astype(F32)
        done = mixed[mine, :, cols(c)].astype(F32) + both
        result[z, mine, :, cols(c)] = done.astype(BF)
        gz_start(1, c)

    def write_out(c):
        if c < NC_BOTH:
            gz_wait(1, c)
        else:
            gx(1, c, 1 - xh).wait_recv()
        out_ref[cols(c), :] = result[:, :, :, cols(c)].reshape(tok, CHUNKS[c][1]).T

    give_back(0)
    give_back(1)
    mixed_across(1 - xh).wait_recv()
    for c in range(NC):
        combine(c)
        if c:
            finish_rows(c - 1)
        ez_done_ex_start(c)
        if c + 2 < NC:
            give_back(c + 2)
    finish_rows(NC - 1)
    for c in range(NC):
        if c >= NC_BOTH:
            gz_done_gx_start(1, c)
        else:
            write_out(c)
    for c in range(NC_BOTH, NC):
        write_out(c)

    mixed_across(xh).wait_send()
    for copy in halo:
        copy.wait_send()
    for c in range(NC):
        for copy in weights[c][1]:
            copy.wait_send()
        rx(c).wait_send()
        ex(c).wait_send()
        gx(0, c, xh).wait_send()
        if c >= NC_BOTH:
            gx(1, c, xh).wait_send()

        rz_all(c).wait_send()
        ez_all(c).wait_send()
        gz_all(0, c).wait_send()
        gz_all(1, c).wait_send()
        group(di, c, 0, NS - 1).wait_send()
        group(re, c, 0, NS - 1).wait_send()


def on_device(
    queries,
    key_rows,
    value_rows,
    sink_logits,
    residual,
    out_weight,
    norm_gain,
    expert_ids,
    route_gates,
    gate_proj,
    up_proj,
    down_proj,
):
    tok, width = residual.shape
    rows = tok // NE
    hid = down_proj.shape[1]
    vmem = pl.BlockSpec(memory_space=pltpu.VMEM)
    hbm = pl.BlockSpec(memory_space=pl.ANY)
    dma = pltpu.SemaphoreType.DMA
    sums = [pltpu.VMEM((NZ, rows, width), BF)] * 3
    slots = pltpu.VMEM((NS, SLOTS, width), BF)
    whole = pltpu.VMEM((NZ, 2, rows, width), BF)
    both = pltpu.VMEM((2, rows, width), BF)
    out = pl.pallas_call(
        layer_kernel,
        out_shape=jax.ShapeDtypeStruct((width, tok), BF),
        in_specs=[vmem] * 5 + [hbm] * 7,
        out_specs=vmem,
        scratch_shapes=[
            pltpu.VMEM((WIN + tok, 2 * HEAD), BF),
            pltpu.VMEM((WIN + tok, 2 * HEAD), BF),
            pltpu.VMEM((width, queries.shape[1]), BF),
            pltpu.VMEM((width, tok), BF),
            pltpu.VMEM((NS // QUAD, QUAD * SLOTS, tok), BF),
            pltpu.VMEM((NS // QUAD, tok, QUAD * SLOTS), BF),
            whole,
        ]
        + sums
        + [whole, both, both]
        + [
            whole,
            both,
            slots,
            slots,
            slots,
            slots,
            pltpu.VMEM((width, 8 * hid), BF),
            pltpu.VMEM((width, 4 * hid), BF),
            pltpu.VMEM((NS // QUAD, QUAD * SLOTS, 8 * hid), F32),
            pltpu.VMEM((NS // QUAD, QUAD * SLOTS, 4 * hid), BF),
            whole,
            whole,
        ]
        + [dma((NC, 6))] * 3
        + [dma((2, NC))] * 8
        + [dma((1,))] * 2
        + [dma((NC,)), dma((NC, NS // QUAD))] * 2
        + [dma((2, NC)), dma((4,)), dma((2,)), dma((2,))],
        compiler_params=pltpu.CompilerParams(
            collective_id=0, has_side_effects=True, vmem_limit_bytes=62 * 1024 * 1024
        ),
    )(
        queries,
        sink_logits.reshape(1, -1),
        norm_gain.reshape(1, width),
        expert_ids.T,
        route_gates.T,
        key_rows,
        value_rows,
        out_weight.T,
        residual.T,
        gate_proj,
        up_proj,
        down_proj.transpose(0, 2, 1),
    )
    return out.T


def solution(mesh):
    in_specs = (
        P("seq", "exp"),
        P("seq", None),
        P("seq", None),
        P("exp"),
        P("seq", None),
        P("exp", None),
        P(),
        P("seq", None),
        P("seq", None),
        P("seq", None, "exp"),
        P("seq", None, "exp"),
        P("seq", "exp", None),
    )
    return jax.shard_map(
        on_device, mesh=mesh, in_specs=in_specs, out_specs=P("seq", None), check_vma=False
    )
```

```python
import functools
import math

import jax
import jax.numpy as jnp
from jax import lax
from jax.experimental import pallas as pl
from jax.experimental.pallas import tpu as pltpu
from jax.sharding import PartitionSpec as P

HQ = 64
HK = 8
HEAD = 64
TOP = 4
WIN = 128
NS = 16
NE = 16
EXPERTS = 64
CAP = 24
SLOTS = 2 * CAP
QUAD = 4
NZ = 8
CUTS = (0, 640, 1280, 1920, 2432, 2880)
LATE_CUTS = (0, 384, 1152, 1920, 2560, 2880)
CHUNKS = tuple(
    tuple((a, b - a) for a, b in zip(cuts, cuts[1:])) for cuts in (CUTS, LATE_CUTS)
)
NC = len(CHUNKS[0])
NC_BOTH = 1
MESH = pl.DeviceIdType.MESH
BF = jnp.bfloat16
F32 = jnp.float32


def layer_kernel(
    query_ref,
    sink_ref,
    gain_ref,
    ids_ref,
    gates_ref,
    key_ref,
    value_ref,
    proj_ref,
    skip_ref,
    gate_ref,
    up_ref,
    down_ref,
    out_ref,
    keys,
    values,
    proj,
    resid,
    pick,
    comb,
    attn,
    xin,
    zsrc,
    zin,
    zin2,
    pair,
    pair_in,
    normed,
    mixed,
    packed,
    arrived,
    outgoing,
    returned,
    w_in,
    w_down,
    acc,
    hidden,
    moe_part,
    result,
    w_local,
    w_send,
    w_recv,
    rx_send,
    rx_recv,
    rz_send,
    rz_recv,
    gx_send,
    gx_recv,
    gz_send,
    gz_recv,
    mx_send,
    mx_recv,
    di_send,
    di_recv,
    re_send,
    re_recv,
    own_sem,
    load_sem,
    halo_send,
    halo_recv,
):
    s = lax.axis_index("seq")
    e = lax.axis_index("exp")
    z = lax.div(e, 2)
    xh = lax.rem(e, 2)
    parity = lax.rem(z + s, 2)
    mate = 2 * lax.rem(z + 1 + (NZ - 2) * parity, NZ) + xh
    across = e + 1 - 2 * xh
    rows = mixed.shape[1]
    quad = lax.div(s, QUAD)
    hid = gate_ref.shape[2]
    tok = NE * rows

    lanes = pl.ds(pl.multiple_of(lax.div(e, 4) * 2 * HEAD, 2 * HEAD), 2 * HEAD)
    loads = [
        pltpu.make_async_copy(src, dst, load_sem.at[i])
        for i, (src, dst) in enumerate(
            (
                (key_ref.at[:, lanes], keys.at[pl.ds(WIN, tok)]),
                (value_ref.at[:, lanes], values.at[pl.ds(WIN, tok)]),
                (proj_ref, proj),
                (skip_ref, resid),
            )
        )
    ]
    for copy in loads:
        copy.start()

    barrier = pltpu.get_barrier_semaphore()

    @pl.loop(1, NE)
    def _(d):
        pl.semaphore_signal(
            barrier, inc=1, device_id={"exp": lax.rem(e + d, NE)}, device_id_type=MESH
        )

    @pl.loop(1, NS)
    def _(d):
        pl.semaphore_signal(
            barrier, inc=1, device_id={"seq": lax.rem(s + d, NS)}, device_id_type=MESH
        )

    def head_of(buf, at):
        both = buf[pl.ds(at, 2 * WIN), :]
        return jnp.where(lax.rem(lax.div(e, 2), 2) == 1, both[:, HEAD:], both[:, :HEAD])

    def context(half):
        heads = query_ref.shape[1] // HEAD
        at = half * WIN
        query = jnp.concatenate(
            [query_ref[at : at + WIN, h * HEAD : (h + 1) * HEAD] for h in range(heads)], 0
        )
        scores = lax.dot_general(
            query, head_of(keys, at), (((1,), (1,)), ((), ())), preferred_element_type=F32
        ) * (1.0 / math.sqrt(HEAD))
        row = lax.rem(lax.broadcasted_iota(jnp.int32, scores.shape, 0), WIN)
        col = lax.broadcasted_iota(jnp.int32, scores.shape, 1)
        allowed = (col > row) & (col <= row + WIN)
        if half == 0:
            allowed = allowed & ((col >= WIN) | (s > 0))
        scores = jnp.where(allowed, scores, -1e30)
        sink = jnp.concatenate(
            [jnp.broadcast_to(sink_ref[:, h : h + 1], (WIN, 1)) for h in range(heads)], 0
        )
        top = jnp.maximum(jnp.max(scores, axis=-1, keepdims=True), sink)
        expo = jnp.exp(scores - top)
        total = jnp.sum(expo, axis=-1, keepdims=True) + jnp.exp(sink - top)
        weights = (expo / total).astype(BF)
        out = jnp.dot(weights, head_of(values, at), preferred_element_type=F32).astype(BF)
        return jnp.concatenate([out[h * WIN : (h + 1) * WIN] for h in range(heads)], 1)

    loads[0].wait()
    loads[1].wait()
    second = context(1)
    pl.semaphore_wait(barrier, NE + NS - 2)

    def rdma(src, dst, send, recv, **where):
        return pltpu.make_async_remote_copy(
            src_ref=src,
            dst_ref=dst,
            send_sem=send,
            recv_sem=recv,
            device_id=where,
            device_id_type=MESH,
        )

    def cols(c, late=0):
        return pl.ds(*CHUNKS[late][c])

    def other(d):
        return lax.rem(z + d, NZ)

    def rx(c):
        return rdma(
            attn.at[:, 1 - xh, :, cols(c)],
            xin.at[:, :, cols(c)],
            rx_send.at[0, c],
            rx_recv.at[0, c],
            exp=across,
        )

    def rz(c, to, frm):
        return rdma(
            zsrc.at[to, :, cols(c)],
            zin.at[frm, :, cols(c)],
            rz_send.at[0, c],
            rz_recv.at[0, c],
            exp=2 * to + xh,
        )

    def rz_all(c):
        part = zin.at[pl.ds(0, NZ - 1), :, cols(c)]
        return rdma(part, part, rz_send.at[0, c], rz_recv.at[0, c], exp=across)

    def rx_done_rz_start(c):
        rx(c).wait_recv()
        both = attn[:, xh, :, cols(c)].astype(F32) + xin[:, :, cols(c)].astype(F32)
        zsrc[:, :, cols(c)] = both.astype(BF)

        @pl.loop(1, NZ)
        def _(d):
            rz(c, other(NZ - d), z).start()

    def rz_sum(c):
        rz_all(c).wait_recv()
        sum_ = zsrc[z, :, cols(c)].astype(F32)
        for d in range(1, NZ):
            sum_ += zin[other(d), :, cols(c)].astype(F32)
        return sum_

    def ez(c, to, frm):
        return rdma(
            moe_part.at[to, :, :, cols(c, 1)],
            zin2.at[frm, :, :, cols(c, 1)],
            rz_send.at[1, c],
            rz_recv.at[1, c],
            exp=2 * to + xh,
        )

    def ez_all(c):
        part = zin2.at[pl.ds(0, NZ - 1), :, :, cols(c, 1)]
        return rdma(part, part, rz_send.at[1, c], rz_recv.at[1, c], exp=across)

    def ez_start(c):
        @pl.loop(1, NZ)
        def _(d):
            ez(c, other(NZ - d), z).start()

    def ex(c):
        return rdma(
            pair.at[:, :, cols(c, 1)],
            pair_in.at[:, :, cols(c, 1)],
            rx_send.at[1, c],
            rx_recv.at[1, c],
            exp=across,
        )

    def ez_done_ex_start(c):
        ez_all(c).wait_recv()
        sum_ = moe_part[z, :, :, cols(c, 1)].astype(F32)
        for d in range(1, NZ):
            sum_ += zin2[other(d), :, :, cols(c, 1)].astype(F32)
        pair[:, :, cols(c, 1)] = sum_.astype(BF)
        ex(c).start()

    def mixed_across(half):
        return rdma(mixed.at[half], mixed.at[half], mx_send.at[0], mx_recv.at[0], exp=across)

    def gz(n, c, to, frm):
        if n == 0:
            block = normed.at[frm, :, :, cols(c)]
        elif c < NC_BOTH:
            block = result.at[frm, :, :, cols(c, 1)]
        else:
            block = result.at[frm, xh, :, cols(c, 1)]
        return rdma(block, block, gz_send.at[n, c], gz_recv.at[n, c], exp=2 * to + xh)

    def gz_start(n, c):
        @pl.loop(1, NZ)
        def _(d):
            gz(n, c, other(NZ - d), z).start()

    def gz_all(n, c):
        if n == 0:
            part = normed.at[pl.ds(0, NZ - 1), :, :, cols(c)]
        elif c < NC_BOTH:
            part = result.at[pl.ds(0, NZ - 1), :, :, cols(c, 1)]
        else:
            part = result.at[pl.ds(0, NZ - 1), xh, :, cols(c, 1)]
        return rdma(part, part, gz_send.at[n, c], gz_recv.at[n, c], exp=across)

    def gx(n, c, half):
        if n == 0:
            block = normed.at[z, half, :, cols(c)]
        else:
            block = result.at[:, half, :, cols(c, 1)]
        return rdma(block, block, gx_send.at[n, c], gx_recv.at[n, c], exp=across)

    def weight_pairs(c):
        keep, give = [], []
        for ref in (gate_ref, up_ref, down_ref):
            for k in range(2):
                at = (0, 2 * hid, 0)[len(keep) // 2] + k * (2 if ref is down_ref else 4) * hid
                buf = w_down if ref is down_ref else w_in
                span = cols(c, int(ref is down_ref))
                keep.append((ref.at[2 * parity + k, span], buf.at[span, pl.ds(at, hid)]))
                give.append((ref.at[2 - 2 * parity + k, span], buf.at[span, pl.ds(at + hid, hid)]))
        keep = [pltpu.make_async_copy(a, b, w_local.at[c, i]) for i, (a, b) in enumerate(keep)]
        give = [
            rdma(a, b, w_send.at[c, i], w_recv.at[c, i], exp=mate) for i, (a, b) in enumerate(give)
        ]
        return keep, give

    weights = [weight_pairs(c) for c in range(NC)]

    queue = [copy for c in range(NC) for copy in weights[c][1][:4]]
    queue += [copy for c in range(NC) for copy in weights[c][1][4:]]

    def give(count):
        for copy in queue[:count]:
            copy.start()
        del queue[:count]

    halo = [
        rdma(
            ref.at[pl.ds(tok - WIN, WIN), lanes],
            buf.at[pl.ds(0, WIN)],
            halo_send.at[i],
            halo_recv.at[i],
            seq=lax.rem(s + 1, NS),
        )
        for i, (ref, buf) in enumerate(((key_ref, keys), (value_ref, values)))
    ]
    for copy in halo:
        copy.start()
    give(4)
    for c in range(NC):
        for copy in weights[c][0]:
            copy.start()
    loads[2].wait()
    for copy in halo:
        copy.wait_recv()
    mixed_heads = jnp.concatenate([context(0), second], 0)
    for c in range(NC):
        part = lax.dot_general(
            mixed_heads, proj[cols(c), :], (((1,), (1,)), ((), ())), preferred_element_type=F32
        )
        attn[:, :, :, cols(c)] = part.astype(BF).reshape(NZ, 2, rows, CHUNKS[0][c][1])
        rx(c).start()

    half = EXPERTS // 2
    index = lax.broadcasted_iota(jnp.int32, (half, tok), 0)
    group_of = lax.div(index, 2)
    mine = 4 * group_of + 2 * lax.rem(group_of + z, 2) + lax.rem(index, 2)
    named = jnp.zeros((half, tok), F32)
    gate_of = jnp.zeros((half, tok), F32)
    for k in range(TOP):
        hit = ids_ref[k : k + 1, :] == mine
        named += jnp.where(hit, 1.0, 0.0)
        gate_of += jnp.where(hit, gates_ref[k : k + 1, :], 0.0)
    earlier = lax.broadcasted_iota(jnp.int32, (tok, tok), 0) < lax.broadcasted_iota(
        jnp.int32, (tok, tok), 1
    )
    count = jnp.dot(
        named.astype(BF), jnp.where(earlier, 1.0, 0.0).astype(BF), preferred_element_type=F32
    )
    slot_of = jnp.where(named > 0.0, count, -1.0).astype(BF)
    gate_of = gate_of.astype(BF)
    for q in range(NS // QUAD):
        shape = (QUAD * SLOTS, half)
        place = lax.div(lax.broadcasted_iota(jnp.int32, shape, 0), CAP) + q * 2 * QUAD
        spread = jnp.where(place == lax.broadcasted_iota(jnp.int32, shape, 1), 1.0, 0.0)
        spread = spread.astype(BF)
        wide = jnp.dot(spread, slot_of, preferred_element_type=F32)
        number = lax.rem(lax.broadcasted_iota(jnp.int32, (QUAD * SLOTS, tok), 0), CAP)
        taken = wide == number.astype(F32)
        gate_wide = jnp.dot(spread, gate_of, preferred_element_type=F32)
        pick[q] = jnp.where(taken, 1.0, 0.0).astype(BF)
        comb[q] = jnp.where(taken, gate_wide, 0.0).T.astype(BF)
    loads[3].wait()

    for c in range(NC):
        rx_done_rz_start(c)
    pick_own = (
        lax.broadcasted_iota(jnp.int32, (rows, tok), 1)
        == e * rows + lax.broadcasted_iota(jnp.int32, (rows, tok), 0)
    ).astype(BF)
    square = jnp.zeros((rows, 1), F32)
    for c in range(NC):
        own = lax.dot_general(
            pick_own,
            resid[cols(c), :],
            (((1,), (1,)), ((), ())),
            preferred_element_type=F32,
        )
        mine = (own + rz_sum(c)).astype(BF)
        mixed[xh, :, cols(c)] = mine
        wide = mine.astype(F32)
        square += jnp.sum(wide * wide, axis=-1, keepdims=True)
    scale = lax.rsqrt(square / mixed.shape[2] + 1e-05)
    for c in range(NC):
        wide = mixed[xh, :, cols(c)].astype(F32)
        normed[z, xh, :, cols(c)] = (wide * scale * gain_ref[cols(c)].reshape(1, -1)).astype(BF)
        gx(0, c, xh).start()
    mixed_across(xh).start()
    for c in range(NC):
        gx(0, c, 1 - xh).wait_recv()
        gz_start(0, c)
    give(len(queue))

    def di(c, to, frm, d=0):
        return rdma(
            packed.at[to, :, cols(c)],
            arrived.at[frm, :, cols(c)],
            di_send.at[c],
            di_recv.at[c, d],
            seq=to,
        )

    def di_own(c):
        return pltpu.make_async_copy(
            packed.at[s, :, cols(c)], arrived.at[s, :, cols(c)], own_sem.at[0, c]
        )

    def re(c, to, frm, d=0):
        return rdma(
            outgoing.at[to, :, cols(c, 1)],
            returned.at[frm, :, cols(c, 1)],
            re_send.at[c],
            re_recv.at[c, d],
            seq=to,
        )

    def re_own(c):
        return pltpu.make_async_copy(
            outgoing.at[s, :, cols(c, 1)], returned.at[s, :, cols(c, 1)], own_sem.at[1, c]
        )

    def peers(d):
        if d:
            q = lax.rem(quad + d, NS // QUAD)
            return [q * QUAD + j for j in range(QUAD)]
        return [quad * QUAD + lax.rem(s + j, QUAD) for j in range(1, QUAD)]

    def put(buf, q, c, block):
        span = cols(c, int(buf is outgoing))
        for j in range(QUAD):
            buf[q * QUAD + j, :, span] = block[j * SLOTS : (j + 1) * SLOTS]

    def start(copy, own, d, c):
        for to in peers(d):
            copy(c, to, s, (NS // QUAD - d) % (NS // QUAD)).start()
        if d == 0:
            own(c).start()

    def group(copy, c, d, count):
        buf = arrived if copy is di else returned
        part = buf.at[pl.ds(0, count), :, cols(c, int(copy is re))]
        send, recv = (di_send, di_recv) if copy is di else (re_send, re_recv)
        return rdma(part, part, send.at[c], recv.at[c, d], exp=across)

    def wait(copy, own, d, c):
        group(copy, c, d, QUAD if d else QUAD - 1).wait_recv()
        if d == 0:
            own(c).wait()

    def pack(c):
        gz_all(0, c).wait_recv()
        full = normed[:, :, :, cols(c)].reshape(tok, CHUNKS[0][c][1])
        for d in (2, 1, 3, 0):
            q = lax.rem(quad + d, NS // QUAD)
            put(packed, q, c, jnp.dot(pick[q], full, preferred_element_type=F32).astype(BF))
            start(di, di_own, d, c)

    for c in range(NC):
        pack(c)

    def activated(block):
        gate = jnp.minimum(block[:, : 2 * hid], 7.0)
        up = jnp.clip(block[:, 2 * hid :], -7.0, 7.0)
        return (up + 1.0) * gate * jax.nn.sigmoid(1.702 * gate)

    slot = lax.rem(lax.broadcasted_iota(jnp.int32, (QUAD * SLOTS, 2 * hid), 0), SLOTS)

    def give_back(c, d, rows_in=None):
        q = lax.rem(quad + d, NS // QUAD)
        block = lax.dot_general(
            hidden[q] if rows_in is None else rows_in,
            w_down[cols(c, 1), :],
            (((1,), (1,)), ((), ())),
            preferred_element_type=F32,
        )
        put(outgoing, q, c, block.astype(BF))

    for c in range(NC):
        for copy in weights[c][0]:
            copy.wait()
        for copy in weights[c][1][:4]:
            copy.wait_recv()
        if c == NC - 1:
            for copy in weights[0][1][4:]:
                copy.wait_recv()
        for d in (0, 1, 3, 2):
            q = lax.rem(quad + d, NS // QUAD)
            wait(di, di_own, d, c)
            x = jnp.concatenate([arrived[q * QUAD + j, :, cols(c)] for j in range(QUAD)], 0)
            add = jnp.dot(x, w_in[cols(c), :], preferred_element_type=F32)
            if c == 0:
                acc[q] = add
            elif c < NC - 1:
                acc[q] += add
            else:
                full = acc[q] + add
                first = jnp.where(slot < CAP, activated(full[:, : 4 * hid]), 0.0)
                second = jnp.where(slot >= CAP, activated(full[:, 4 * hid :]), 0.0)
                units = jnp.concatenate([first, second], 1).astype(BF)
                hidden[q] = units
                give_back(0, d, units)
                start(re, re_own, d, 0)

    def combine(c):
        sum_ = None
        for d in (0, 1, 3, 2):
            q = lax.rem(quad + d, NS // QUAD)
            wait(re, re_own, d, c)
            y = jnp.concatenate([returned[q * QUAD + j, :, cols(c, 1)] for j in range(QUAD)], 0)
            add = jnp.dot(comb[q], y, preferred_element_type=F32)
            sum_ = add if sum_ is None else sum_ + add
        moe_part[:, :, :, cols(c, 1)] = sum_.astype(BF).reshape(NZ, 2, rows, CHUNKS[1][c][1])
        ez_start(c)

    def finish_rows(c):
        ex(c).wait_recv()
        mine = slice(None) if c < NC_BOTH else xh
        both = pair[mine, :, cols(c, 1)].astype(F32) + pair_in[mine, :, cols(c, 1)].astype(F32)
        done = mixed[mine, :, cols(c, 1)].astype(F32) + both
        result[z, mine, :, cols(c, 1)] = done.astype(BF)
        gz_start(1, c)

    def write_out(c):
        if c < NC_BOTH:
            gz_all(1, c).wait_recv()
        else:
            gx(1, c, 1 - xh).wait_recv()
        out_ref[cols(c, 1), :] = result[:, :, :, cols(c, 1)].reshape(tok, CHUNKS[1][c][1]).T

    def prepare(c):
        for copy in weights[c][1][4:]:
            copy.wait_recv()
        for d in (2, 1, 3, 0):
            give_back(c, d)

    def send_back(c):
        for d in (2, 1, 3, 0):
            start(re, re_own, d, c)

    prepare(1)
    send_back(1)
    mixed_across(1 - xh).wait_recv()
    for c in range(NC):
        if c + 2 < NC:
            prepare(c + 2)
        combine(c)
        if c + 2 < NC:
            send_back(c + 2)
        if c >= 2:
            finish_rows(c - 2)
        if c == NC - 1:
            finish_rows(c - 1)
        ez_done_ex_start(c)
    finish_rows(NC - 1)
    for c in range(NC):
        if c >= NC_BOTH:
            gz_all(1, c).wait_recv()
            gx(1, c, xh).start()
        else:
            write_out(c)
    for c in range(NC_BOTH, NC):
        write_out(c)

    mixed_across(xh).wait_send()
    for copy in halo:
        copy.wait_send()
    for c in range(NC):
        for copy in weights[c][1]:
            copy.wait_send()
        rx(c).wait_send()
        ex(c).wait_send()
        gx(0, c, xh).wait_send()
        if c >= NC_BOTH:
            gx(1, c, xh).wait_send()

        rz_all(c).wait_send()
        ez_all(c).wait_send()
        gz_all(0, c).wait_send()
        gz_all(1, c).wait_send()
        group(di, c, 0, NS - 1).wait_send()
        group(re, c, 0, NS - 1).wait_send()


def on_device(
    queries,
    key_rows,
    value_rows,
    sink_logits,
    residual,
    out_weight,
    norm_gain,
    expert_ids,
    route_gates,
    gate_proj,
    up_proj,
    down_proj,
):
    tok, width = residual.shape
    rows = tok // NE
    hid = down_proj.shape[1]
    vmem = pl.BlockSpec(memory_space=pltpu.VMEM)
    hbm = pl.BlockSpec(memory_space=pl.ANY)
    dma = pltpu.SemaphoreType.DMA
    sums = [pltpu.VMEM((NZ, rows, width), BF)] * 3
    slots = pltpu.VMEM((NS, SLOTS, width), BF)
    whole = pltpu.VMEM((NZ, 2, rows, width), BF)
    both = pltpu.VMEM((2, rows, width), BF)
    out = pl.pallas_call(
        layer_kernel,
        out_shape=jax.ShapeDtypeStruct((width, tok), BF),
        in_specs=[vmem] * 5 + [hbm] * 7,
        out_specs=vmem,
        scratch_shapes=[
            pltpu.VMEM((WIN + tok, 2 * HEAD), BF),
            pltpu.VMEM((WIN + tok, 2 * HEAD), BF),
            pltpu.VMEM((width, queries.shape[1]), BF),
            pltpu.VMEM((width, tok), BF),
            pltpu.VMEM((NS // QUAD, QUAD * SLOTS, tok), BF),
            pltpu.VMEM((NS // QUAD, tok, QUAD * SLOTS), BF),
            whole,
        ]
        + sums
        + [whole, both, both]
        + [
            whole,
            both,
            slots,
            slots,
            slots,
            slots,
            pltpu.VMEM((width, 8 * hid), BF),
            pltpu.VMEM((width, 4 * hid), BF),
            pltpu.VMEM((NS // QUAD, QUAD * SLOTS, 8 * hid), F32),
            pltpu.VMEM((NS // QUAD, QUAD * SLOTS, 4 * hid), BF),
            whole,
            whole,
        ]
        + [dma((NC, 6))] * 3
        + [dma((2, NC))] * 8
        + [dma((1,))] * 2
        + [dma((NC,)), dma((NC, NS // QUAD))] * 2
        + [dma((2, NC)), dma((4,)), dma((2,)), dma((2,))],
        compiler_params=pltpu.CompilerParams(
            collective_id=0, has_side_effects=True, vmem_limit_bytes=62 * 1024 * 1024
        ),
    )(
        queries,
        sink_logits.reshape(1, -1),
        norm_gain,
        expert_ids.T,
        route_gates.T,
        key_rows,
        value_rows,
        out_weight.T,
        residual.T,
        gate_proj,
        up_proj,
        down_proj.transpose(0, 2, 1),
    )
    return out.T


def solution(mesh):
    in_specs = (
        P("seq", "exp"),
        P("seq", None),
        P("seq", None),
        P("exp"),
        P("seq", None),
        P("exp", None),
        P(),
        P("seq", None),
        P("seq", None),
        P("seq", None, "exp"),
        P("seq", None, "exp"),
        P("seq", "exp", None),
    )
    return jax.shard_map(
        on_device, mesh=mesh, in_specs=in_specs, out_specs=P("seq", None), check_vma=False
    )
```

```python
import functools
import math

import jax
import jax.numpy as jnp
from jax import lax
from jax.experimental import pallas as pl
from jax.experimental.pallas import tpu as pltpu
from jax.sharding import PartitionSpec as P

HQ = 64
HK = 8
HEAD = 64
TOP = 4
WIN = 128
NS = 16
NE = 16
EXPERTS = 64
CAP = 24
SLOTS = 2 * CAP
QUAD = 4
NZ = 8
CUTS = (0, 640, 1280, 1920, 2432, 2880)
LATE_CUTS = (0, 384, 1152, 1920, 2560, 2880)
CHUNKS = tuple(
    tuple((a, b - a) for a, b in zip(cuts, cuts[1:])) for cuts in (CUTS, LATE_CUTS)
)
NC = len(CHUNKS[0])
NC_BOTH = 1
MESH = pl.DeviceIdType.MESH
BF = jnp.bfloat16
F32 = jnp.float32


def layer_kernel(
    query_ref,
    sink_ref,
    gain_ref,
    ids_ref,
    gates_ref,
    key_ref,
    value_ref,
    proj_ref,
    skip_ref,
    gate_ref,
    up_ref,
    down_ref,
    out_ref,
    keys,
    values,
    proj,
    resid,
    pick,
    comb,
    attn,
    xin,
    zsrc,
    zin,
    zin2,
    pair,
    pair_in,
    normed,
    mixed,
    packed,
    arrived,
    outgoing,
    returned,
    w_in,
    w_down,
    acc,
    hidden,
    moe_part,
    result,
    w_local,
    w_send,
    w_recv,
    rx_send,
    rx_recv,
    rz_send,
    rz_recv,
    gx_send,
    gx_recv,
    gz_send,
    gz_recv,
    mx_send,
    mx_recv,
    di_send,
    di_recv,
    re_send,
    re_recv,
    own_sem,
    load_sem,
    halo_send,
    halo_recv,
):
    s = lax.axis_index("seq")
    e = lax.axis_index("exp")
    z = lax.div(e, 2)
    xh = lax.rem(e, 2)
    parity = lax.rem(z + s, 2)
    mate = 2 * lax.rem(z + 1 + (NZ - 2) * parity, NZ) + xh
    across = e + 1 - 2 * xh
    rows = mixed.shape[1]
    quad = lax.div(s, QUAD)
    hid = gate_ref.shape[2]
    tok = NE * rows

    lanes = pl.ds(pl.multiple_of(lax.div(e, 4) * 2 * HEAD, 2 * HEAD), 2 * HEAD)
    loads = [
        pltpu.make_async_copy(src, dst, load_sem.at[i])
        for i, (src, dst) in enumerate(
            (
                (key_ref.at[:, lanes], keys.at[pl.ds(WIN, tok)]),
                (value_ref.at[:, lanes], values.at[pl.ds(WIN, tok)]),
                (proj_ref, proj),
                (skip_ref, resid),
            )
        )
    ]
    for copy in loads:
        copy.start()

    barrier = pltpu.get_barrier_semaphore()

    @pl.loop(1, NE)
    def _(d):
        pl.semaphore_signal(
            barrier, inc=1, device_id={"exp": lax.rem(e + d, NE)}, device_id_type=MESH
        )

    @pl.loop(1, NS)
    def _(d):
        pl.semaphore_signal(
            barrier, inc=1, device_id={"seq": lax.rem(s + d, NS)}, device_id_type=MESH
        )

    def head_of(buf, at):
        both = buf[pl.ds(at, 2 * WIN), :]
        return jnp.where(lax.rem(lax.div(e, 2), 2) == 1, both[:, HEAD:], both[:, :HEAD])

    def context(half):
        heads = query_ref.shape[1] // HEAD
        at = half * WIN
        query = jnp.concatenate(
            [query_ref[at : at + WIN, h * HEAD : (h + 1) * HEAD] for h in range(heads)], 0
        )
        scores = lax.dot_general(
            query, head_of(keys, at), (((1,), (1,)), ((), ())), preferred_element_type=F32
        ) * (1.0 / math.sqrt(HEAD))
        row = lax.rem(lax.broadcasted_iota(jnp.int32, scores.shape, 0), WIN)
        col = lax.broadcasted_iota(jnp.int32, scores.shape, 1)
        allowed = (col > row) & (col <= row + WIN)
        if half == 0:
            allowed = allowed & ((col >= WIN) | (s > 0))
        scores = jnp.where(allowed, scores, -1e30)
        sink = jnp.concatenate(
            [jnp.broadcast_to(sink_ref[:, h : h + 1], (WIN, 1)) for h in range(heads)], 0
        )
        top = jnp.maximum(jnp.max(scores, axis=-1, keepdims=True), sink)
        expo = jnp.exp(scores - top)
        total = jnp.sum(expo, axis=-1, keepdims=True) + jnp.exp(sink - top)
        weights = (expo / total).astype(BF)
        out = jnp.dot(weights, head_of(values, at), preferred_element_type=F32).astype(BF)
        return jnp.concatenate([out[h * WIN : (h + 1) * WIN] for h in range(heads)], 1)

    loads[0].wait()
    loads[1].wait()
    second = context(1)
    pl.semaphore_wait(barrier, NE + NS - 2)

    def rdma(src, dst, send, recv, **where):
        return pltpu.make_async_remote_copy(
            src_ref=src,
            dst_ref=dst,
            send_sem=send,
            recv_sem=recv,
            device_id=where,
            device_id_type=MESH,
        )

    def cols(c, late=0):
        return pl.ds(*CHUNKS[late][c])

    def other(d):
        return lax.rem(z + d, NZ)

    def rx(c):
        return rdma(
            attn.at[:, 1 - xh, :, cols(c)],
            xin.at[:, :, cols(c)],
            rx_send.at[0, c],
            rx_recv.at[0, c],
            exp=across,
        )

    def rz(c, to, frm):
        return rdma(
            zsrc.at[to, :, cols(c)],
            zin.at[frm, :, cols(c)],
            rz_send.at[0, c],
            rz_recv.at[0, c],
            exp=2 * to + xh,
        )

    def rz_all(c):
        part = zin.at[pl.ds(0, NZ - 1), :, cols(c)]
        return rdma(part, part, rz_send.at[0, c], rz_recv.at[0, c], exp=across)

    def rx_done_rz_start(c):
        rx(c).wait_recv()
        both = attn[:, xh, :, cols(c)].astype(F32) + xin[:, :, cols(c)].astype(F32)
        zsrc[:, :, cols(c)] = both.astype(BF)

        @pl.loop(1, NZ)
        def _(d):
            rz(c, other(NZ - d), z).start()

    def rz_sum(c):
        rz_all(c).wait_recv()
        sum_ = zsrc[z, :, cols(c)].astype(F32)
        for d in range(1, NZ):
            sum_ += zin[other(d), :, cols(c)].astype(F32)
        return sum_

    def ez(c, to, frm):
        return rdma(
            moe_part.at[to, :, :, cols(c, 1)],
            zin2.at[frm, :, :, cols(c, 1)],
            rz_send.at[1, c],
            rz_recv.at[1, c],
            exp=2 * to + xh,
        )

    def ez_all(c):
        part = zin2.at[pl.ds(0, NZ - 1), :, :, cols(c, 1)]
        return rdma(part, part, rz_send.at[1, c], rz_recv.at[1, c], exp=across)

    def ez_start(c):
        @pl.loop(1, NZ)
        def _(d):
            ez(c, other(NZ - d), z).start()

    def ex(c):
        return rdma(
            pair.at[:, :, cols(c, 1)],
            pair_in.at[:, :, cols(c, 1)],
            rx_send.at[1, c],
            rx_recv.at[1, c],
            exp=across,
        )

    def ez_done_ex_start(c):
        ez_all(c).wait_recv()
        sum_ = moe_part[z, :, :, cols(c, 1)].astype(F32)
        for d in range(1, NZ):
            sum_ += zin2[other(d), :, :, cols(c, 1)].astype(F32)
        pair[:, :, cols(c, 1)] = sum_.astype(BF)
        ex(c).start()

    def mixed_across(half):
        return rdma(mixed.at[half], mixed.at[half], mx_send.at[0], mx_recv.at[0], exp=across)

    def gz(n, c, to, frm):
        if n == 0:
            block = normed.at[frm, :, :, cols(c)]
        elif c < NC_BOTH:
            block = result.at[frm, :, :, cols(c, 1)]
        else:
            block = result.at[frm, xh, :, cols(c, 1)]
        return rdma(block, block, gz_send.at[n, c], gz_recv.at[n, c], exp=2 * to + xh)

    def gz_start(n, c):
        @pl.loop(1, NZ)
        def _(d):
            gz(n, c, other(NZ - d), z).start()

    def gz_all(n, c):
        if n == 0:
            part = normed.at[pl.ds(0, NZ - 1), :, :, cols(c)]
        elif c < NC_BOTH:
            part = result.at[pl.ds(0, NZ - 1), :, :, cols(c, 1)]
        else:
            part = result.at[pl.ds(0, NZ - 1), xh, :, cols(c, 1)]
        return rdma(part, part, gz_send.at[n, c], gz_recv.at[n, c], exp=across)

    def gx(n, c, half):
        if n == 0:
            block = normed.at[z, half, :, cols(c)]
        else:
            block = result.at[:, half, :, cols(c, 1)]
        return rdma(block, block, gx_send.at[n, c], gx_recv.at[n, c], exp=across)

    def weight_pairs(c):
        keep, give = [], []
        for ref in (gate_ref, up_ref, down_ref):
            for k in range(2):
                at = (0, 2 * hid, 0)[len(keep) // 2] + k * (2 if ref is down_ref else 4) * hid
                buf = w_down if ref is down_ref else w_in
                span = cols(c, int(ref is down_ref))
                keep.append((ref.at[2 * parity + k, span], buf.at[span, pl.ds(at, hid)]))
                give.append((ref.at[2 - 2 * parity + k, span], buf.at[span, pl.ds(at + hid, hid)]))
        keep = [pltpu.make_async_copy(a, b, w_local.at[c, i]) for i, (a, b) in enumerate(keep)]
        give = [
            rdma(a, b, w_send.at[c, i], w_recv.at[c, i], exp=mate) for i, (a, b) in enumerate(give)
        ]
        return keep, give

    weights = [weight_pairs(c) for c in range(NC)]

    queue = [copy for c in range(NC) for copy in weights[c][1][:4]]
    queue += [copy for c in range(NC) for copy in weights[c][1][4:]]

    def give(count):
        for copy in queue[:count]:
            copy.start()
        del queue[:count]

    halo = [
        rdma(
            ref.at[pl.ds(tok - WIN, WIN), lanes],
            buf.at[pl.ds(0, WIN)],
            halo_send.at[i],
            halo_recv.at[i],
            seq=lax.rem(s + 1, NS),
        )
        for i, (ref, buf) in enumerate(((key_ref, keys), (value_ref, values)))
    ]
    for copy in halo:
        copy.start()
    give(4)
    for c in range(NC):
        for copy in weights[c][0]:
            copy.start()
    loads[2].wait()
    for copy in halo:
        copy.wait_recv()
    mixed_heads = jnp.concatenate([context(0), second], 0)
    for c in range(NC):
        part = lax.dot_general(
            mixed_heads, proj[cols(c), :], (((1,), (1,)), ((), ())), preferred_element_type=F32
        )
        attn[:, :, :, cols(c)] = part.astype(BF).reshape(NZ, 2, rows, CHUNKS[0][c][1])
        rx(c).start()

    half = EXPERTS // 2
    index = lax.broadcasted_iota(jnp.int32, (half, tok), 0)
    group_of = lax.div(index, 2)
    mine = 4 * group_of + 2 * lax.rem(group_of + z, 2) + lax.rem(index, 2)
    named = jnp.zeros((half, tok), F32)
    gate_of = jnp.zeros((half, tok), F32)
    for k in range(TOP):
        hit = ids_ref[k : k + 1, :] == mine
        named += jnp.where(hit, 1.0, 0.0)
        gate_of += jnp.where(hit, gates_ref[k : k + 1, :], 0.0)
    earlier = lax.broadcasted_iota(jnp.int32, (tok, tok), 0) < lax.broadcasted_iota(
        jnp.int32, (tok, tok), 1
    )
    count = jnp.dot(
        named.astype(BF), jnp.where(earlier, 1.0, 0.0).astype(BF), preferred_element_type=F32
    )
    slot_of = jnp.where(named > 0.0, count, -1.0).astype(BF)
    gate_of = gate_of.astype(BF)
    for q in range(NS // QUAD):
        shape = (QUAD * SLOTS, half)
        place = lax.div(lax.broadcasted_iota(jnp.int32, shape, 0), CAP) + q * 2 * QUAD
        spread = jnp.where(place == lax.broadcasted_iota(jnp.int32, shape, 1), 1.0, 0.0)
        spread = spread.astype(BF)
        wide = jnp.dot(spread, slot_of, preferred_element_type=F32)
        number = lax.rem(lax.broadcasted_iota(jnp.int32, (QUAD * SLOTS, tok), 0), CAP)
        taken = wide == number.astype(F32)
        gate_wide = jnp.dot(spread, gate_of, preferred_element_type=F32)
        pick[q] = jnp.where(taken, 1.0, 0.0).astype(BF)
        comb[q] = jnp.where(taken, gate_wide, 0.0).T.astype(BF)
    loads[3].wait()

    for c in range(NC):
        rx_done_rz_start(c)
    pick_own = (
        lax.broadcasted_iota(jnp.int32, (rows, tok), 1)
        == e * rows + lax.broadcasted_iota(jnp.int32, (rows, tok), 0)
    ).astype(BF)
    square = jnp.zeros((rows, 1), F32)
    for c in range(NC):
        own = lax.dot_general(
            pick_own,
            resid[cols(c), :],
            (((1,), (1,)), ((), ())),
            preferred_element_type=F32,
        )
        mine = (own + rz_sum(c)).astype(BF)
        mixed[xh, :, cols(c)] = mine
        wide = mine.astype(F32)
        square += jnp.sum(wide * wide, axis=-1, keepdims=True)
    scale = lax.rsqrt(square / mixed.shape[2] + 1e-05)
    for c in range(NC):
        wide = mixed[xh, :, cols(c)].astype(F32)
        normed[z, xh, :, cols(c)] = (wide * scale * gain_ref[cols(c)].reshape(1, -1)).astype(BF)
        gx(0, c, xh).start()
    mixed_across(xh).start()
    for c in range(NC):
        gx(0, c, 1 - xh).wait_recv()
        gz_start(0, c)
    give(len(queue))

    def di(c, to, frm, d=0):
        return rdma(
            packed.at[to, :, cols(c)],
            arrived.at[frm, :, cols(c)],
            di_send.at[c],
            di_recv.at[c, d],
            seq=to,
        )

    def di_own(c):
        return pltpu.make_async_copy(
            packed.at[s, :, cols(c)], arrived.at[s, :, cols(c)], own_sem.at[0, c]
        )

    def re(c, to, frm, d=0):
        return rdma(
            outgoing.at[to, :, cols(c, 1)],
            returned.at[frm, :, cols(c, 1)],
            re_send.at[c],
            re_recv.at[c, d],
            seq=to,
        )

    def re_own(c):
        return pltpu.make_async_copy(
            outgoing.at[s, :, cols(c, 1)], returned.at[s, :, cols(c, 1)], own_sem.at[1, c]
        )

    def peers(d):
        if d:
            q = lax.rem(quad + d, NS // QUAD)
            return [q * QUAD + j for j in range(QUAD)]
        return [quad * QUAD + lax.rem(s + j, QUAD) for j in range(1, QUAD)]

    def put(buf, q, c, block):
        span = cols(c, int(buf is outgoing))
        for j in range(QUAD):
            buf[q * QUAD + j, :, span] = block[j * SLOTS : (j + 1) * SLOTS]

    def start(copy, own, d, c):
        for to in peers(d):
            copy(c, to, s, (NS // QUAD - d) % (NS // QUAD)).start()
        if d == 0:
            own(c).start()

    def group(copy, c, d, count):
        buf = arrived if copy is di else returned
        part = buf.at[pl.ds(0, count), :, cols(c, int(copy is re))]
        send, recv = (di_send, di_recv) if copy is di else (re_send, re_recv)
        return rdma(part, part, send.at[c], recv.at[c, d], exp=across)

    def wait(copy, own, d, c):
        group(copy, c, d, QUAD if d else QUAD - 1).wait_recv()
        if d == 0:
            own(c).wait()

    def pack(c):
        gz_all(0, c).wait_recv()
        full = normed[:, :, :, cols(c)].reshape(tok, CHUNKS[0][c][1])
        for d in (2, 1, 3, 0):
            q = lax.rem(quad + d, NS // QUAD)
            put(packed, q, c, jnp.dot(pick[q], full, preferred_element_type=F32).astype(BF))
            start(di, di_own, d, c)

    for c in range(NC):
        pack(c)

    def activated(block):
        gate = jnp.minimum(block[:, : 2 * hid], 7.0)
        up = jnp.clip(block[:, 2 * hid :], -7.0, 7.0)
        return (up + 1.0) * gate * jax.nn.sigmoid(1.702 * gate)

    slot = lax.rem(lax.broadcasted_iota(jnp.int32, (QUAD * SLOTS, 2 * hid), 0), SLOTS)

    def give_back(c, d, rows_in=None):
        q = lax.rem(quad + d, NS // QUAD)
        block = lax.dot_general(
            hidden[q] if rows_in is None else rows_in,
            w_down[cols(c, 1), :],
            (((1,), (1,)), ((), ())),
            preferred_element_type=F32,
        )
        put(outgoing, q, c, block.astype(BF))

    for c in range(NC):
        for copy in weights[c][0]:
            copy.wait()
        for copy in weights[c][1][:4]:
            copy.wait_recv()
        if c == NC - 1:
            for copy in weights[0][1][4:]:
                copy.wait_recv()
        for d in (0, 1, 3, 2):
            q = lax.rem(quad + d, NS // QUAD)
            wait(di, di_own, d, c)
            x = jnp.concatenate([arrived[q * QUAD + j, :, cols(c)] for j in range(QUAD)], 0)
            add = jnp.dot(x, w_in[cols(c), :], preferred_element_type=F32)
            if c == 0:
                acc[q] = add
            elif c < NC - 1:
                acc[q] += add
            else:
                full = acc[q] + add
                first = jnp.where(slot < CAP, activated(full[:, : 4 * hid]), 0.0)
                second = jnp.where(slot >= CAP, activated(full[:, 4 * hid :]), 0.0)
                units = jnp.concatenate([first, second], 1).astype(BF)
                hidden[q] = units
                give_back(0, d, units)
                start(re, re_own, d, 0)

    def combine(c):
        sum_ = None
        for d in (0, 1, 3, 2):
            q = lax.rem(quad + d, NS // QUAD)
            wait(re, re_own, d, c)
            y = jnp.concatenate([returned[q * QUAD + j, :, cols(c, 1)] for j in range(QUAD)], 0)
            add = jnp.dot(comb[q], y, preferred_element_type=F32)
            sum_ = add if sum_ is None else sum_ + add
        moe_part[:, :, :, cols(c, 1)] = sum_.astype(BF).reshape(NZ, 2, rows, CHUNKS[1][c][1])
        ez_start(c)

    def finish_rows(c):
        ex(c).wait_recv()
        mine = slice(None) if c < NC_BOTH else xh
        both = pair[mine, :, cols(c, 1)].astype(F32) + pair_in[mine, :, cols(c, 1)].astype(F32)
        done = mixed[mine, :, cols(c, 1)].astype(F32) + both
        result[z, mine, :, cols(c, 1)] = done.astype(BF)
        gz_start(1, c)

    def write_out(c):
        if c < NC_BOTH:
            gz_all(1, c).wait_recv()
        else:
            gx(1, c, 1 - xh).wait_recv()
        out_ref[cols(c, 1), :] = result[:, :, :, cols(c, 1)].reshape(tok, CHUNKS[1][c][1]).T

    def across_next(c):
        gz_all(1, c).wait_recv()
        gx(1, c, xh).start()

    def prepare(c):
        for copy in weights[c][1][4:]:
            copy.wait_recv()
        for d in (2, 1, 3, 0):
            give_back(c, d)

    def send_back(c):
        for d in (2, 1, 3, 0):
            start(re, re_own, d, c)

    prepare(1)
    send_back(1)
    mixed_across(1 - xh).wait_recv()
    for c in range(NC):
        if c + 2 < NC:
            prepare(c + 2)
        combine(c)
        if c + 2 < NC:
            send_back(c + 2)
        if c >= 2:
            finish_rows(c - 2)
        if c == NC - 1:
            finish_rows(c - 1)
            across_next(NC_BOTH)
            write_out(0)
        ez_done_ex_start(c)
    across_next(NC_BOTH + 1)
    finish_rows(NC - 1)
    for c in range(1, NC_BOTH + 1):
        write_out(c)
    for c in range(NC_BOTH + 2, NC):
        across_next(c)
    for c in range(NC_BOTH + 1, NC):
        write_out(c)

    mixed_across(xh).wait_send()
    for copy in halo:
        copy.wait_send()
    for c in range(NC):
        for copy in weights[c][1]:
            copy.wait_send()
        rx(c).wait_send()
        ex(c).wait_send()
        gx(0, c, xh).wait_send()
        if c >= NC_BOTH:
            gx(1, c, xh).wait_send()

        rz_all(c).wait_send()
        ez_all(c).wait_send()
        gz_all(0, c).wait_send()
        gz_all(1, c).wait_send()
        group(di, c, 0, NS - 1).wait_send()
        group(re, c, 0, NS - 1).wait_send()


def on_device(
    queries,
    key_rows,
    value_rows,
    sink_logits,
    residual,
    out_weight,
    norm_gain,
    expert_ids,
    route_gates,
    gate_proj,
    up_proj,
    down_proj,
):
    tok, width = residual.shape
    rows = tok // NE
    hid = down_proj.shape[1]
    vmem = pl.BlockSpec(memory_space=pltpu.VMEM)
    hbm = pl.BlockSpec(memory_space=pl.ANY)
    dma = pltpu.SemaphoreType.DMA
    sums = [pltpu.VMEM((NZ, rows, width), BF)] * 3
    slots = pltpu.VMEM((NS, SLOTS, width), BF)
    whole = pltpu.VMEM((NZ, 2, rows, width), BF)
    both = pltpu.VMEM((2, rows, width), BF)
    out = pl.pallas_call(
        layer_kernel,
        out_shape=jax.ShapeDtypeStruct((width, tok), BF),
        in_specs=[vmem] * 5 + [hbm] * 7,
        out_specs=vmem,
        scratch_shapes=[
            pltpu.VMEM((WIN + tok, 2 * HEAD), BF),
            pltpu.VMEM((WIN + tok, 2 * HEAD), BF),
            pltpu.VMEM((width, queries.shape[1]), BF),
            pltpu.VMEM((width, tok), BF),
            pltpu.VMEM((NS // QUAD, QUAD * SLOTS, tok), BF),
            pltpu.VMEM((NS // QUAD, tok, QUAD * SLOTS), BF),
            whole,
        ]
        + sums
        + [whole, both, both]
        + [
            whole,
            both,
            slots,
            slots,
            slots,
            slots,
            pltpu.VMEM((width, 8 * hid), BF),
            pltpu.VMEM((width, 4 * hid), BF),
            pltpu.VMEM((NS // QUAD, QUAD * SLOTS, 8 * hid), F32),
            pltpu.VMEM((NS // QUAD, QUAD * SLOTS, 4 * hid), BF),
            whole,
            whole,
        ]
        + [dma((NC, 6))] * 3
        + [dma((2, NC))] * 8
        + [dma((1,))] * 2
        + [dma((NC,)), dma((NC, NS // QUAD))] * 2
        + [dma((2, NC)), dma((4,)), dma((2,)), dma((2,))],
        compiler_params=pltpu.CompilerParams(
            collective_id=0, has_side_effects=True, vmem_limit_bytes=62 * 1024 * 1024
        ),
    )(
        queries,
        sink_logits.reshape(1, -1),
        norm_gain,
        expert_ids.T,
        route_gates.T,
        key_rows,
        value_rows,
        out_weight.T,
        residual.T,
        gate_proj,
        up_proj,
        down_proj.transpose(0, 2, 1),
    )
    return out.T


def solution(mesh):
    in_specs = (
        P("seq", "exp"),
        P("seq", None),
        P("seq", None),
        P("exp"),
        P("seq", None),
        P("exp", None),
        P(),
        P("seq", None),
        P("seq", None),
        P("seq", None, "exp"),
        P("seq", None, "exp"),
        P("seq", "exp", None),
    )
    return jax.shard_map(
        on_device, mesh=mesh, in_specs=in_specs, out_specs=P("seq", None), check_vma=False
    )
```
